256 devices in a mesh: row: 16 (over z, core), col: 16 (over x, y).
Axes of the slice: x: 4, y: 4, z: 8, core: 2. Of those that a mesh axis runs over, the one named last changes fastest.
Arguments:
- train_weight: bfloat16 [4, 4608, 8192], P(None, 'row', 'col')
- src_map: int32 [64], replicated, may hold values from 0 to 63, as said below
- tgt_map: int32 [64], replicated, may hold values from 0 to 63, as said below
- probe: bfloat16 [8192, 4608], P('row'), may hold values from -6 to 6
Outputs:
- codes: bfloat16 [4, 4608, 8192], P(None, None, 'col')
- peaks: float32 [4, 64], P(None, 'col')
- checked: bfloat16 [4, 8192, 8192], P(None, 'row', 'col')
The draws below stay inside these ranges and needn't reach their ends.
Inputs may be any that keep to these rules, and one draw needn't show every extreme that they name: src_map is a permutation of 0 to 63. tgt_map is a permutation of 0 to 63. Call column k the slots k * 4 to (k + 1) * 4 - 1 of a map, and let C = 16. There are three different offsets a, b, c in 0 to C - 1, the same for every column, of which one is C / 2 and one is C - 1: the heads of training column k stand in serving columns (k - a) mod C (2 of them), (k - b) mod C (one) and (k - c) mod C (one).
All inputs are finite; a program needn't handle non-finite values. Where the reference program divides by a largest or mean magnitude, that divisor is 1e-20 or more.
Results may differ from the reference program's by a relative error of at most 0.0049.
Values may be sent and summed in bfloat16 or wider, within the bound.
A program may use at most 128 MiB of HBM per device.

```python
import jax
import jax.numpy as jnp

D = 4608
HDIM = 128
HCOL = 4
LAYERS = 4
TOKENS = 8192
N_COL = 16


def head_maps(key):
    heads_all = HCOL * N_COL
    keys = jax.random.split(jax.random.fold_in(key, 17), 6)
    source = jax.random.permutation(keys[0], heads_all).astype(jnp.int32)
    half = N_COL // 2
    before_one = jnp.array([N_COL - 1], jnp.int32)
    picked = jax.random.randint(keys[5], (1,), 0, N_COL - 2).astype(jnp.int32)
    third = jnp.where(picked < half, picked, picked + 1).astype(jnp.int32)
    three = jnp.concatenate([jnp.array([half], jnp.int32), before_one, third])
    offsets = three[jax.random.permutation(keys[4], 3)].astype(jnp.int32)
    pattern = jnp.array([0, 0, 1, 2], jnp.int32)
    roles = jax.vmap(lambda single: jax.random.permutation(single, 4))(jax.random.split(keys[2], N_COL)).astype(jnp.int32)
    locals_order = jax.vmap(lambda single: jax.random.permutation(single, 4))(jax.random.split(keys[3], N_COL)).astype(jnp.int32)
    targets = jnp.arange(N_COL, dtype=jnp.int32)[:, None]
    shifted = offsets[pattern[roles]]
    from_col = (targets + shifted) % N_COL
    local_slot = locals_order[from_col, roles]
    target = source[(from_col * HCOL + local_slot).reshape(-1)]
    return (source, target.astype(jnp.int32))


def draw_src_map(key, part):
    return head_maps(key)[0]


def draw_tgt_map(key, part):
    return head_maps(key)[1]


def draw_train_weight(key, part):
    keys = jax.random.split(jax.random.fold_in(key, 5), 3)
    heads_all = HCOL * N_COL
    head_scale = jnp.exp(jax.random.uniform(keys[1], (LAYERS, 1, heads_all, 1), jnp.float32, jnp.log(0.3), jnp.log(3.0)))
    row_scale = jnp.exp(jax.random.uniform(keys[2], (1, D, 1, 1), jnp.float32, jnp.log(0.4), jnp.log(4.0)))
    base = jax.random.normal(keys[0], (LAYERS, D, heads_all, HDIM), jnp.float32)
    weights = base * head_scale * row_scale / jnp.sqrt(jnp.float32(D))
    return weights.reshape(LAYERS, D, heads_all * HDIM).astype(jnp.bfloat16)


def block_scale(stream_key, shape, cuts, smallest, high):
    def one(position, shards_of):
        heights = jax.random.uniform(jax.random.fold_in(jax.random.fold_in(stream_key, 6), position), (shards_of,), jnp.float32, smallest / len(cuts), high / len(cuts))
        return jnp.repeat(jnp.exp(heights), shape[position] // shards_of).reshape((-1,) + (1,) * (len(shape) - position - 1))

    loudness = one(*cuts[0])
    for cut in cuts[1:]:
        loudness = loudness * one(*cut)
    return loudness


def bell_draw(stream_key, shape, spread, most, cuts=(), kind=jnp.bfloat16):
    loudness = block_scale(stream_key, shape, cuts, -0.22, 0.18) if cuts else 1.0
    entries = jax.random.normal(stream_key, shape, jnp.float32) * spread * loudness
    return jnp.minimum(jnp.maximum(entries, -most), most).astype(kind)


def setup_inputs(seed: int = 0) -> dict:
    streams_of = jax.random.split(jax.random.key(seed), 5)
    return {
        "train_weight": draw_train_weight(jax.random.fold_in(streams_of[4], 71), 0),
        "src_map": draw_src_map(jax.random.fold_in(streams_of[4], 71), 0),
        "tgt_map": draw_tgt_map(jax.random.fold_in(streams_of[4], 71), 0),
        "probe": bell_draw(streams_of[3], (TOKENS, D), 1.0, 6.0, ((0, 16),)),
    }


def reference(train_weight, src_map, tgt_map, probe):
    heads_all = src_map.shape[0]
    slot_ids = jnp.arange(heads_all, dtype=jnp.int32)
    matched = (src_map[None, :] == tgt_map[:, None]).astype(jnp.int32)
    source = jnp.sum(matched * slot_ids[None, :], axis=1).astype(jnp.int32)
    heads_four = train_weight.reshape(LAYERS, D, heads_all, HDIM)
    served = jnp.take(heads_four, source, axis=2)
    peaks = jnp.max(jnp.abs(served.astype(jnp.float32)), axis=(1, 3))
    codes = (served.astype(jnp.float32) / (peaks[:, None, :, None] + 1e-6)).astype(jnp.bfloat16)
    codes = codes.reshape(LAYERS, D, heads_all * HDIM)
    results = []
    for layer in range(LAYERS):
        projected = jnp.dot(probe, codes[layer], preferred_element_type=jnp.float32)
        scaled = projected * jnp.repeat(peaks[layer], HDIM)[None, :]
        results.append(scaled.astype(jnp.bfloat16))
    return codes, peaks, jnp.stack(results)
```

```python
import functools

import jax
import jax.numpy as jnp
from jax import lax
from jax.experimental import pallas as pl
from jax.experimental.pallas import tpu as pltpu
from jax.sharding import PartitionSpec as P

HDIM = 128
MESH = pl.DeviceIdType.MESH
LAYERS = 4
NZ = 8
NCOL = 16
HEADS = 64
PER = 4
EPS = 1e-06


def rem(a, n):
    return lax.rem(a, n)


def send_classes(src_ref, tgt_ref, col):
    heads = [src_ref[col * PER + i] for i in range(PER)]

    def look(t, found):
        head = tgt_ref[t]
        return tuple(jnp.where(head == h, t, f) for h, f in zip(heads, found))

    zero = jnp.int32(0)
    found = lax.fori_loop(0, HEADS, look, (zero,) * PER, unroll=8)
    shifts = [rem(f // PER - col + NCOL, NCOL) for f in found]

    def first(test):
        at = jnp.int32(PER - 1)
        for i in range(PER - 2, -1, -1):
            at = jnp.where(test(shifts[i]), i, at)
        return at

    at_a = first(lambda s: s == 8)
    at_b = first(lambda s: s == 1)
    at_s = first(lambda s: (s != 8) & (s != 1))
    at_e = 6 - at_a - at_b - at_s

    def pick(at):
        value = shifts[PER - 1]
        for i in range(PER - 2, -1, -1):
            value = jnp.where(at == i, shifts[i], value)
        return value

    return at_a, at_b, at_s, at_e, pick(at_s), pick(at_e)


def recv_classes(src_ref, tgt_ref, col):
    wanted = [tgt_ref[col * PER + j] for j in range(PER)]

    def look(t, found):
        head = src_ref[t]
        return tuple(jnp.where(head == h, t, f) for h, f in zip(wanted, found))

    zero = jnp.int32(0)
    found = lax.fori_loop(0, HEADS, look, (zero,) * PER, unroll=8)
    classes = []
    for f in found:
        from_col = f // PER
        place = rem(f, PER)
        shift = rem(col - from_col + NCOL, NCOL)
        later = jnp.int32(0)
        for i in range(PER - 1):
            head = src_ref[from_col * PER + i]
            mine = jnp.int32(0)
            for h in wanted:
                mine = jnp.where(head == h, 1, mine)
            later = jnp.where(i < place, jnp.maximum(later, mine), later)
        kind = jnp.where(shift == 8, 0, jnp.where(shift == 1, 1, 2))
        classes.append(jnp.where(later == 1, 3, kind))
    return classes


def gather_kernel(
    src_ref, tgt_ref, w_hbm, probe_hbm,
    c_ref, acc_ref, pk_ref,
    g_ref, probe_ref, w_ref, sb_ref, mx_ref, mine_ref, rk_ref,
    x1a, x1b, x1c, x1d, x2a, x2b, x2c, x2d,
    y1a, y1b, y1c, y1d, y2a, y2b, y2c, y2d,
    w_sem, p_sem, ab_recv, ab_send, xy_recv, xy_send, z_recv, z_send,
    own_recv, own_send, d_recv, d_send, mx_recv, mx_send,
):
    x1, x2 = (x1a, x1b, x1c, x1d), (x2a, x2b, x2c, x2d)
    y1, y2 = (y1a, y1b, y1c, y1d), (y2a, y2b, y2c, y2d)
    row = lax.axis_index("row")
    col = lax.axis_index("col")
    z, core = row // 2, rem(row, 2)
    depth = w_ref.shape[1]
    quad = 4 * depth

    def w_copy(l):
        return pltpu.make_async_copy(w_hbm.at[l], w_ref.at[l], w_sem.at[l])

    def p_copy():
        return pltpu.make_async_copy(probe_hbm, probe_ref, p_sem)

    barrier = pltpu.get_barrier_semaphore()
    for d in range(1, 16):
        pl.semaphore_signal(barrier, inc=1, device_id=(rem(row + d, 16), col), device_id_type=MESH)
    for d in (8, 1, 15, 4, 12):
        pl.semaphore_signal(barrier, inc=1, device_id=(row, rem(col + d, NCOL)), device_id_type=MESH)
    for l in range(LAYERS):
        w_copy(l).start()
    p_copy().start()

    at_a, at_b, at_s, at_e, s_by, e_by = send_classes(src_ref, tgt_ref, col)
    s_x, s_y = rem((s_by + 1) // 4, 4), rem(s_by + 1, 4) - 1
    e_x, e_y = rem((e_by + 2) // 4, 4), rem(e_by + 2, 4) - 2
    x1_s = jnp.where(s_x == 0, 0, jnp.where(s_x == 3, 2, 1))
    x1_e = jnp.where(e_x == 0, 0, jnp.where(e_x == 1, 1, 2))
    x2_s, x2_e = jnp.where(s_x == 2, 1, 0), jnp.where(e_x == 2, 1, 0)
    y1_s = jnp.where(s_y == 0, 0, jnp.where(s_y == -1, 2, 1))
    y1_e = jnp.where(e_y == 0, 0, jnp.where(e_y == 1, 1, 2))
    y2_s, y2_e = jnp.where(s_y == 2, 1, 0), jnp.where(e_y == -2, 1, 0)

    def choose(at, values):
        out = values[-1]
        for i in range(len(values) - 2, -1, -1):
            out = jnp.where(at == i, values[i], out)
        return out

    def head(l, at):
        return choose(at, [w_ref[l, :, i * HDIM:(i + 1) * HDIM] for i in range(PER)])

    for l in range(LAYERS):
        w_copy(l).wait()
        sb_ref[l, 0] = head(l, at_a)
        sb_ref[l, 1] = head(l, at_b)
        x1[l][0, 0] = head(l, at_s)
        x1[l][0, 1] = head(l, at_e)

    pl.semaphore_wait(barrier, 20)

    def to_col(src, dst, sems, at, by):
        send, recv = sems
        return pltpu.make_async_remote_copy(
            src_ref=src, dst_ref=dst, send_sem=send.at[at], recv_sem=recv.at[at],
            device_id=(row, rem(col + by, NCOL)), device_id_type=MESH,
        )

    def a_copy(l):
        return to_col(sb_ref.at[l, 0], g_ref.at[0, 0, l, 0], (ab_send, ab_recv), (l, 0), 8)

    def b_copy(l):
        return to_col(sb_ref.at[l, 1], g_ref.at[0, 0, l, 1], (ab_send, ab_recv), (l, 1), 1)

    def x1_copy(l, way):
        return to_col(x1[l].at[0], x1[l].at[1 + way], (xy_send, xy_recv), (0, l, way), (4, 12)[way])

    def x2_copy(l, half):
        return to_col(x2[l].at[0, half], x2[l].at[1, half], (xy_send, xy_recv), (1, l, half), (4, 12)[half])

    def y1_copy(l, way):
        return to_col(y1[l].at[0], y1[l].at[1 + way], (xy_send, xy_recv), (2, l, way), (1, 15)[way])

    def y2_copy(l, half):
        return to_col(y2[l].at[0, half], y2[l].at[1, half], (xy_send, xy_recv), (3, l, half), (1, 15)[half])

    for l in range(LAYERS):
        a_copy(l).start()
        b_copy(l).start()
    for l in range(LAYERS):
        for way in range(2):
            x1_copy(l, way).start()

    def z_copy(way, d, q, slot):
        to = rem(z + (1, NZ - 1)[way], NZ) * 2 + core
        return pltpu.make_async_remote_copy(
            src_ref=g_ref.at[d, 0, q], dst_ref=g_ref.at[(d + (NZ - 1, 1)[way]) % NZ, 0, q],
            send_sem=z_send.at[way, slot], recv_sem=z_recv.at[way, slot],
            device_id=(to, col), device_id_type=MESH,
        )

    def z_arrival(way, d, q, slot):
        return z_copy(way, (d + (1, NZ - 1)[way]) % NZ, q, slot)

    def d_copy(d, q, sems, at):
        send, recv = sems
        return pltpu.make_async_remote_copy(
            src_ref=g_ref.at[d, 0, q], dst_ref=g_ref.at[d, 1, q],
            send_sem=send.at[at], recv_sem=recv.at[at],
            device_id=(z * 2 + 1 - core, col), device_id_type=MESH,
        )

    def d_own(q):
        return d_copy(0, q, (own_send, own_recv), q)

    def d_passed(way, slot, d, q):
        return d_copy(d, q, (d_send, d_recv), (way, slot))

    def send_own(q):
        for way in range(2):
            z_copy(way, 0, q, q // 4 * 14 + q % 4).start()
        d_own(q).start()

    def place(way, slot):
        group, i = slot // 14, slot % 14
        hop = i // 4 + 1
        q = group * 4 + (i % 4 if i < 12 else 2 * (i - 12) + way)
        return (NZ - hop, hop)[way], q

    def ring(slot):
        i = slot % 14
        for way in range(2):
            d, q = place(way, slot)
            z_arrival(way, d, q, slot).wait_recv()
            if i < 8:
                z_copy(way, d, q, slot + 4).start()
            elif i < 12 and i % 2 == way:
                z_copy(way, d, q, slot - i + 12 + (i - 8) // 2).start()
            d_passed(way, slot, d, q).start()

    def beside(slot):
        for way in range(2):
            d_passed(way, slot, *place(way, slot)).wait_recv()

    def biggest(group):
        rows = []
        for half in range(2):
            for l in range(LAYERS):
                block = g_ref[0, 0, group * 4 + l, half]
                rows.append(jnp.max(jnp.abs(block.astype(jnp.float32)), axis=0, keepdims=True))
        mine_ref[group] = jnp.concatenate(rows, axis=0)

    def mx_copy(group, by):
        return pltpu.make_async_remote_copy(
            src_ref=mine_ref.at[group], dst_ref=mx_ref.at[group, by],
            send_sem=mx_send.at[group, by], recv_sem=mx_recv.at[group, by],
            device_id=(rem(row + by, 16), col), device_id_type=MESH,
        )

    def settle(group):
        for by in range(1, 16):
            mx_copy(group, by).wait_recv()
        top = mine_ref[group]
        for rb in range(1, 16):
            top = jnp.maximum(top, mx_ref[group, rb])
        top = jnp.broadcast_to(jnp.max(top, axis=1, keepdims=True), top.shape)
        pk_ref[group] = top
        rk_ref[group] = 1.0 / ((top + EPS) * 0.0625)

    even = rem(z, 2) == 0

    def unit(group, t, l):
        p = rem(z // 2 + (0, -1, 1, 2)[t] * (1 - 2 * rem(z, 2)) + 4, 4)
        q = group * 4 + l
        start = pl.multiple_of(p * quad, HDIM)
        for half in range(2):
            scale = rk_ref[group, half * 4 + l:half * 4 + l + 1, :]
            for d in ((0, 1), (-1, -2), (2, 3), (-3, 4))[t]:
                for other in range(2):
                    block = g_ref[d % NZ, other, q, half]
                    if d % 4:
                        block = jnp.where(even, block, g_ref[-d % NZ, other, q, half])
                    at = start + rem(z + d + NZ, 2) * (2 * depth) + (core + other - 2 * core * other) * depth
                    c_ref[q, half, pl.ds(pl.multiple_of(at, 16), depth), :] = (
                        (block.astype(jnp.float32) * 0.0625) * scale
                    ).astype(jnp.bfloat16)
        both = jnp.concatenate(
            [c_ref[q, 0, pl.ds(start, quad), :], c_ref[q, 1, pl.ds(start, quad), :]], axis=1
        )
        acc_ref[q] += jnp.dot(
            probe_ref[:, pl.ds(start, quad)], both, preferred_element_type=jnp.float32
        )

    for l in range(LAYERS):
        for half, copy in enumerate((a_copy, b_copy)):
            copy(l).wait_recv()
        send_own(l)

    @pl.loop(0, 8)
    def _(q):
        acc_ref[q] = jnp.zeros(acc_ref.shape[1:], jnp.float32)

    biggest(0)

    for i in range(15):
        if i == 1:
            for by in range(1, 16):
                mx_copy(0, by).start()
        l = i - 4
        sends = []
        if 0 <= l < 4:
            for way in range(2):
                x1_copy(l, way).wait_recv()
            x2[l][0, 0] = choose(x1_s, [x1[l][i, 0] for i in range(3)])
            x2[l][0, 1] = choose(x1_e, [x1[l][i, 1] for i in range(3)])
            sends += [x2_copy(l, 0), x2_copy(l, 1)]
        l = i - 7
        if 0 <= l < 4:
            for half in range(2):
                x2_copy(l, half).wait_recv()
            y1[l][0, 0] = choose(x2_s, [x2[l][i, 0] for i in range(2)])
            y1[l][0, 1] = choose(x2_e, [x2[l][i, 1] for i in range(2)])
            sends += [y1_copy(l, 0), y1_copy(l, 1)]
        l = i - 9
        if 0 <= l < 4:
            for way in range(2):
                y1_copy(l, way).wait_recv()
            y2[l][0, 0] = choose(y1_s, [y1[l][i, 0] for i in range(3)])
            y2[l][0, 1] = choose(y1_e, [y1[l][i, 1] for i in range(3)])
            sends += [y2_copy(l, 0), y2_copy(l, 1)]
        l = i - 11
        own = None
        if 0 <= l < 4:
            for half in range(2):
                y2_copy(l, half).wait_recv()
            g_ref[0, 0, 4 + l, 0] = choose(y2_s, [y2[l][i, 0] for i in range(2)])
            g_ref[0, 0, 4 + l, 1] = choose(y2_e, [y2[l][i, 1] for i in range(2)])
            own = 4 + l
        if i > 0:
            beside(i - 1)
        for copy in sends:
            copy.start()
        if own is not None:
            send_own(own)
        ring(i)

    p_copy().wait()
    biggest(1)
    settle(0)
    for q in range(4):
        d_own(q).wait_recv()

    for by in range(1, 16):
        mx_copy(1, by).start()

    def units(group, t, first, last):
        for l in range(first, last):
            unit(group, t, l)

    work = {15: (0, 0, 0, 4), 16: (0, 1, 0, 4), 17: (0, 2, 0, 4), 18: (0, 3, 0, 4)}
    work.update({21: (1, 0, 0, 4), 22: (1, 1, 0, 4), 24: (1, 2, 0, 2), 26: (1, 2, 2, 4)})
    work.update({27: (1, 3, 0, 2), 28: (1, 3, 2, 4)})
    for slot in range(15, 29):
        beside(slot - 1)
        if slot < 28:
            ring(slot)
        if slot == 21:
            settle(1)
            for q in range(4, 8):
                d_own(q).wait_recv()
        if slot in work:
            units(*work[slot])

    for q in range(8):
        d_own(q).wait_send()
    for slot in range(28):
        for way in range(2):
            d, q = place(way, slot)
            d_passed(way, slot, d, q).wait_send()
            z_arrival(way, d, q, slot).wait_send()
    for l in range(LAYERS):
        a_copy(l).wait_send()
        b_copy(l).wait_send()
        for way in range(2):
            x1_copy(l, way).wait_send()
            x2_copy(l, way).wait_send()
            y1_copy(l, way).wait_send()
            y2_copy(l, way).wait_send()
    for group in range(2):
        for by in range(1, 16):
            mx_copy(group, by).wait_send()


def output_kernel(
    src_ref, tgt_ref, c_ref, acc_ref, pk_ref,
    codes_hbm, peaks_ref, checked_hbm,
    chk_ref, sem, chk_sem,
):
    col = lax.axis_index("col")
    classes = recv_classes(src_ref, tgt_ref, col)
    slots = []
    for c in range(4):
        at = jnp.int32(0)
        for j in range(1, PER):
            at = jnp.where(classes[j] == c, j, at)
        slots.append(at)

    def lanes(c):
        return pl.ds(pl.multiple_of(slots[c] * HDIM, HDIM), HDIM)

    copies = []
    for l in range(LAYERS):
        for c in range(4):
            copy = pltpu.make_async_copy(
                c_ref.at[c // 2 * 4 + l, c % 2], codes_hbm.at[l, :, lanes(c)], sem.at[l, c]
            )
            copy.start()
            copies.append(copy)
    for l in range(LAYERS):
        for c in range(4):
            half = c % 2
            scale = pk_ref[c // 2, half * 4 + l:half * 4 + l + 1, :]
            block = acc_ref[c // 2 * 4 + l, :, half * HDIM:(half + 1) * HDIM]
            chk_ref[l, c] = (block * scale).astype(jnp.bfloat16)
            copy = pltpu.make_async_copy(
                chk_ref.at[l, c], checked_hbm.at[l, :, lanes(c)], chk_sem.at[l, c]
            )
            copy.start()
            copies.append(copy)
    lane = lax.broadcasted_iota(jnp.int32, (LAYERS, HDIM), 1)
    out = jnp.zeros((LAYERS, HDIM), jnp.float32)
    for c in range(4):
        half = c % 2
        out = jnp.where(lane == slots[c], pk_ref[c // 2, half * 4:half * 4 + 4, :], out)
    peaks_ref[...] = out[:, :PER]
    for copy in copies:
        copy.wait()


def per_device(train_weight, src_map, tgt_map, probe):
    layers, depth, width = train_weight.shape
    tokens, model = probe.shape
    bf16, f32 = jnp.bfloat16, jnp.float32
    smem = pl.BlockSpec(memory_space=pltpu.SMEM)
    vmem = pl.BlockSpec(memory_space=pltpu.VMEM)
    hbm = pl.BlockSpec(memory_space=pl.ANY)
    three = pltpu.VMEM((3, 2, depth, HDIM), bf16)
    two = pltpu.VMEM((2, 2, depth, HDIM), bf16)
    dma = pltpu.SemaphoreType.DMA
    c, acc, pk = pl.pallas_call(
        gather_kernel,
        name="gather_codes",
        out_shape=(
            pltpu.VMEM((8, 2, model, HDIM), bf16),
            pltpu.VMEM((8, tokens, 2 * HDIM), f32),
            pltpu.VMEM((2, 8, HDIM), f32),
        ),
        in_specs=[smem, smem, hbm, hbm],
        out_specs=(vmem, vmem, vmem),
        scratch_shapes=[
            pltpu.VMEM((NZ, 2, 8, 2, depth, HDIM), bf16),
            pltpu.VMEM((tokens, model), bf16),
            pltpu.VMEM((layers, depth, width), bf16),
            pltpu.VMEM((layers, 2, depth, HDIM), bf16),
            pltpu.VMEM((2, 16, 8, HDIM), f32),
            pltpu.VMEM((2, 8, HDIM), f32),
            pltpu.VMEM((2, 8, HDIM), f32),
        ]
        + [three] * 4 + [two] * 4 + [three] * 4 + [two] * 4
        + [
            dma((4,)), dma, dma((4, 2)), dma((4, 2)), dma((4, 4, 2)), dma((4, 4, 2)),
            dma((2, 28)), dma((2, 28)), dma((8,)), dma((8,)), dma((2, 28)), dma((2, 28)),
            dma((2, 16)), dma((2, 16)),
        ],
        compiler_params=pltpu.CompilerParams(
            collective_id=0, has_side_effects=True, vmem_limit_bytes=36 * 1024 * 1024
        ),
    )(src_map, tgt_map, train_weight, probe)
    return pl.pallas_call(
        output_kernel,
        name="write_outputs",
        out_shape=(
            jax.ShapeDtypeStruct((layers, model, width), bf16),
            jax.ShapeDtypeStruct((layers, PER), f32),
            jax.ShapeDtypeStruct((layers, tokens, width), bf16),
        ),
        in_specs=[smem, smem, vmem, vmem, vmem],
        out_specs=(hbm, vmem, hbm),
        scratch_shapes=[
            pltpu.VMEM((layers, 4, tokens, HDIM), bf16),
            dma((4, 4)),
            dma((4, 4)),
        ],
        compiler_params=pltpu.CompilerParams(vmem_limit_bytes=8 * 1024 * 1024),
    )(src_map, tgt_map, c, acc, pk)


def solution(mesh):
    in_specs = (P(None, "row", "col"), P(), P(), P("row", None))
    out_specs = (P(None, None, "col"), P(None, "col"), P(None, "row", "col"))
    return jax.shard_map(
        per_device, mesh=mesh, in_specs=in_specs, out_specs=out_specs, check_vma=False
    )
```

```python
import functools

import jax
import jax.numpy as jnp
from jax import lax
from jax.experimental import pallas as pl
from jax.experimental.pallas import tpu as pltpu
from jax.sharding import PartitionSpec as P

HDIM = 128
MESH = pl.DeviceIdType.MESH
LAYERS = 4
NZ = 8
NCOL = 16
HEADS = 64
PER = 4
EPS = 1e-06


def rem(a, n):
    return lax.rem(a, n)


def send_classes(src_ref, tgt_ref, col):
    heads = [src_ref[col * PER + i] for i in range(PER)]

    def look(t, found):
        head = tgt_ref[t]
        return tuple(jnp.where(head == h, t, f) for h, f in zip(heads, found))

    zero = jnp.int32(0)
    found = lax.fori_loop(0, HEADS, look, (zero,) * PER, unroll=8)
    shifts = [rem(f // PER - col + NCOL, NCOL) for f in found]

    def first(test):
        at = jnp.int32(PER - 1)
        for i in range(PER - 2, -1, -1):
            at = jnp.where(test(shifts[i]), i, at)
        return at

    at_a = first(lambda s: s == 8)
    at_b = first(lambda s: s == 1)
    at_s = first(lambda s: (s != 8) & (s != 1))
    at_e = 6 - at_a - at_b - at_s

    def pick(at):
        value = shifts[PER - 1]
        for i in range(PER - 2, -1, -1):
            value = jnp.where(at == i, shifts[i], value)
        return value

    return at_a, at_b, at_s, at_e, pick(at_s), pick(at_e)


def recv_classes(src_ref, tgt_ref, col):
    wanted = [tgt_ref[col * PER + j] for j in range(PER)]

    def look(t, found):
        head = src_ref[t]
        return tuple(jnp.where(head == h, t, f) for h, f in zip(wanted, found))

    zero = jnp.int32(0)
    found = lax.fori_loop(0, HEADS, look, (zero,) * PER, unroll=8)
    classes = []
    for f in found:
        from_col = f // PER
        place = rem(f, PER)
        shift = rem(col - from_col + NCOL, NCOL)
        later = jnp.int32(0)
        for i in range(PER - 1):
            head = src_ref[from_col * PER + i]
            mine = jnp.int32(0)
            for h in wanted:
                mine = jnp.where(head == h, 1, mine)
            later = jnp.where(i < place, jnp.maximum(later, mine), later)
        kind = jnp.where(shift == 8, 0, jnp.where(shift == 1, 1, 2))
        classes.append(jnp.where(later == 1, 3, kind))
    return classes


def gather_kernel(
    src_ref, tgt_ref, w_hbm, probe_hbm,
    c_ref, acc_ref, pk_ref, last_ref,
    g_ref, probe_ref, w_ref, sb_ref, mx_ref, mine_ref, rk_ref,
    x1a, x1b, x1c, x1d, x2a, x2b, x2c, x2d,
    y1a, y1b, y1c, y1d, y2a, y2b, y2c, y2d,
    w_sem, p_sem, ab_recv, xy_recv, z_recv, own_recv, d_recv, mx_recv,
    xy_send, z_send, d_send, mx_send,
):
    x1, x2 = (x1a, x1b, x1c, x1d), (x2a, x2b, x2c, x2d)
    y1, y2 = (y1a, y1b, y1c, y1d), (y2a, y2b, y2c, y2d)
    row = lax.axis_index("row")
    col = lax.axis_index("col")
    z, core = row // 2, rem(row, 2)
    depth = w_ref.shape[1]
    quad = 4 * depth

    def w_copy(l):
        return pltpu.make_async_copy(w_hbm.at[l], w_ref.at[l], w_sem.at[l])

    def p_copy():
        return pltpu.make_async_copy(probe_hbm, probe_ref, p_sem)

    barrier = pltpu.get_barrier_semaphore()
    for d in range(1, 16):
        pl.semaphore_signal(barrier, inc=1, device_id=(rem(row + d, 16), col), device_id_type=MESH)
    for d in (8, 1, 15, 4, 12):
        pl.semaphore_signal(barrier, inc=1, device_id=(row, rem(col + d, NCOL)), device_id_type=MESH)
    for l in range(LAYERS):
        w_copy(l).start()
    p_copy().start()

    at_a, at_b, at_s, at_e, s_by, e_by = send_classes(src_ref, tgt_ref, col)
    s_x, s_y = rem((s_by + 1) // 4, 4), rem(s_by + 1, 4) - 1
    e_x, e_y = rem((e_by + 2) // 4, 4), rem(e_by + 2, 4) - 2
    x1_s = jnp.where(s_x == 0, 0, jnp.where(s_x == 3, 2, 1))
    x1_e = jnp.where(e_x == 0, 0, jnp.where(e_x == 1, 1, 2))
    x2_s, x2_e = jnp.where(s_x == 2, 1, 0), jnp.where(e_x == 2, 1, 0)
    y1_s = jnp.where(s_y == 0, 0, jnp.where(s_y == -1, 2, 1))
    y1_e = jnp.where(e_y == 0, 0, jnp.where(e_y == 1, 1, 2))
    y2_s, y2_e = jnp.where(s_y == 2, 1, 0), jnp.where(e_y == -2, 1, 0)

    def choose(at, values):
        out = values[-1]
        for i in range(len(values) - 2, -1, -1):
            out = jnp.where(at == i, values[i], out)
        return out

    def head(l, at):
        return choose(at, [w_ref[l, :, i * HDIM:(i + 1) * HDIM] for i in range(PER)])

    for l in range(LAYERS):
        w_copy(l).wait()
        sb_ref[l, 0] = head(l, at_a)
        sb_ref[l, 1] = head(l, at_b)
        x1[l][0, 0] = head(l, at_s)
        x1[l][0, 1] = head(l, at_e)

    @pl.loop(0, 8)
    def _(q):
        acc_ref[q] = jnp.zeros(acc_ref.shape[1:], jnp.float32)

    pl.semaphore_wait(barrier, 20)

    def total(part, send, recv):
        return pltpu.make_async_remote_copy(
            src_ref=part, dst_ref=part, send_sem=send, recv_sem=recv,
            device_id=(row, rem(col + 1, NCOL)), device_id_type=MESH,
        )

    def to_col(src, dst, recv, by):
        return pltpu.make_async_remote_copy(
            src_ref=src, dst_ref=dst, send_sem=xy_send, recv_sem=recv,
            device_id=(row, rem(col + by, NCOL)), device_id_type=MESH,
        )

    def a_copy(l):
        return to_col(sb_ref.at[l, 0], g_ref.at[0, 0, 2 + l // 2, l % 2], ab_recv.at[l, 0], 8)

    def b_copy(l):
        return to_col(sb_ref.at[l, 1], g_ref.at[0, 0, l // 2, l % 2], ab_recv.at[l, 1], 1)

    def wide_copy(stage, buffer, l, way, by):
        return to_col(buffer[l].at[0], buffer[l].at[1 + way], xy_recv.at[stage, l], by[way])

    def half_copy(stage, buffer, l, half, by):
        return to_col(buffer[l].at[0, half], buffer[l].at[1, half], xy_recv.at[stage, l], by[half])

    def shifted(stage, buffer, l):
        part = buffer[l].at[pl.ds(0, 2)] if stage % 2 == 0 else buffer[l].at[0]
        total(part, xy_send, xy_recv.at[stage, l]).wait_recv()

    for l in range(LAYERS):
        b_copy(l).start()
        a_copy(l).start()
    for l in range(LAYERS):
        for way in range(2):
            wide_copy(0, x1, l, way, (4, 12)).start()

    def z_copy(way, d, at, slot):
        to = rem(z + (1, NZ - 1)[way], NZ) * 2 + core
        return pltpu.make_async_remote_copy(
            src_ref=g_ref.at[(d, 0) + at], dst_ref=g_ref.at[((d + (NZ - 1, 1)[way]) % NZ, 0) + at],
            send_sem=z_send, recv_sem=z_recv.at[slot],
            device_id=(to, col), device_id_type=MESH,
        )

    def d_copy(d, q, recv):
        return pltpu.make_async_remote_copy(
            src_ref=g_ref.at[d, 0, q], dst_ref=g_ref.at[d, 1, q],
            send_sem=d_send, recv_sem=recv,
            device_id=(z * 2 + 1 - core, col), device_id_type=MESH,
        )

    def send_own(q, half=None):
        at = (q,) if half is None else (q, half)
        for way in range(2):
            z_copy(way, 0, at, q // 4 * 14 + q % 4).start()
        if half != 0:
            d_copy(0, q, own_recv.at[q // 4]).start()

    def own_beside(group):
        total(g_ref.at[0, 0, pl.ds(0, 4)], d_send, own_recv.at[group]).wait_recv()

    def place(way, slot):
        group, i = slot // 14, slot % 14
        hop = i // 4 + 1
        q = group * 4 + (i % 4 if i < 12 else 2 * (i - 12) + way)
        return (NZ - hop, hop)[way], q

    def ring(slot):
        i = slot % 14
        total(g_ref.at[0, 0, pl.ds(0, 2)], z_send, z_recv.at[slot]).wait_recv()
        for way in range(2):
            d, q = place(way, slot)
            if i < 8:
                z_copy(way, d, (q,), slot + 4).start()
            elif i < 12 and i % 2 == way:
                z_copy(way, d, (q,), slot - i + 12 + (i - 8) // 2).start()
        for way in range(2):
            d, q = place(way, slot)
            d_copy(d, q, d_recv.at[slot]).start()

    def beside(slot):
        total(g_ref.at[0, 0, pl.ds(0, 2)], d_send, d_recv.at[slot]).wait_recv()

    def biggest(group):
        rows = []
        for half in range(2):
            for l in range(LAYERS):
                block = g_ref[0, 0, group * 4 + l, half]
                rows.append(jnp.max(jnp.abs(block.astype(jnp.float32)), axis=0, keepdims=True))
        mine_ref[group] = jnp.concatenate(rows, axis=0)

    def mx_copy(group, by):
        return pltpu.make_async_remote_copy(
            src_ref=mine_ref.at[group], dst_ref=mx_ref.at[group, by],
            send_sem=mx_send, recv_sem=mx_recv.at[group],
            device_id=(rem(row + by, 16), col), device_id_type=MESH,
        )

    def settle(group):
        total(mx_ref.at[group, pl.ds(1, 15)], mx_send, mx_recv.at[group]).wait_recv()
        top = mine_ref[group]
        for rb in range(1, 16):
            top = jnp.maximum(top, mx_ref[group, rb])
        top = jnp.broadcast_to(jnp.max(top, axis=1, keepdims=True), top.shape)
        pk_ref[group] = top
        rk_ref[group] = 1.0 / ((top + EPS) * 0.0625)

    even = rem(z, 2) == 0

    def unit(group, t, l):
        p = rem(z // 2 + (0, -1, 1, 2)[t] * (1 - 2 * rem(z, 2)) + 4, 4)
        q = group * 4 + l
        start = pl.multiple_of(p * quad, HDIM)
        for half in range(2):
            scale = rk_ref[group, half * 4 + l:half * 4 + l + 1, :]
            for d in ((0, 1), (-1, -2), (2, 3), (-3, 4))[t]:
                for other in range(2):
                    block = g_ref[d % NZ, other, q, half]
                    if d % 4:
                        block = jnp.where(even, block, g_ref[-d % NZ, other, q, half])
                    at = start + rem(z + d + NZ, 2) * (2 * depth) + (core + other - 2 * core * other) * depth
                    c_ref[q, half, pl.ds(pl.multiple_of(at, 16), depth), :] = (
                        (block.astype(jnp.float32) * 0.0625) * scale
                    ).astype(jnp.bfloat16)
        if group == 1 and t == 3:
            return
        both = jnp.concatenate(
            [c_ref[q, 0, pl.ds(start, quad), :], c_ref[q, 1, pl.ds(start, quad), :]], axis=1
        )
        acc_ref[q] += jnp.dot(
            probe_ref[:, pl.ds(start, quad)], both, preferred_element_type=jnp.float32
        )

    def took(kind, l):
        (a_copy, b_copy)[kind](l).wait_recv()
        send_own(2 * (1 - kind) + l // 2, l % 2)

    took(1, 0)
    took(1, 1)
    took(0, 0)
    took(1, 2)
    took(1, 3)
    took(0, 1)
    ring(0)
    took(0, 2)
    beside(0)
    ring(1)
    took(0, 3)
    biggest(0)

    for i in range(2, 15):
        if i == 3:
            for by in range(1, 16):
                mx_copy(0, by).start()
        l = i - 4
        sends = []
        if 0 <= l < 4:
            shifted(0, x1, l)
            x2[l][0, 0] = choose(x1_s, [x1[l][k, 0] for k in range(3)])
            x2[l][0, 1] = choose(x1_e, [x1[l][k, 1] for k in range(3)])
            sends += [half_copy(1, x2, l, half, (4, 12)) for half in range(2)]
        l = i - 7
        if 0 <= l < 4:
            shifted(1, x2, l)
            y1[l][0, 0] = choose(x2_s, [x2[l][k, 0] for k in range(2)])
            y1[l][0, 1] = choose(x2_e, [x2[l][k, 1] for k in range(2)])
            sends += [wide_copy(2, y1, l, way, (1, 15)) for way in range(2)]
        l = i - 9
        if 0 <= l < 4:
            shifted(2, y1, l)
            y2[l][0, 0] = choose(y1_s, [y1[l][k, 0] for k in range(3)])
            y2[l][0, 1] = choose(y1_e, [y1[l][k, 1] for k in range(3)])
            sends += [half_copy(3, y2, l, half, (1, 15)) for half in range(2)]
        l = i - 11
        own = None
        if 0 <= l < 4:
            shifted(3, y2, l)
            g_ref[0, 0, 4 + l, 0] = choose(y2_s, [y2[l][k, 0] for k in range(2)])
            g_ref[0, 0, 4 + l, 1] = choose(y2_e, [y2[l][k, 1] for k in range(2)])
            own = 4 + l
        beside(i - 1)
        for copy in sends:
            copy.start()
        if own is not None:
            send_own(own)
        ring(i)

    p_copy().wait()
    last_ref[...] = probe_ref[:, pl.ds(pl.multiple_of(rem(z // 2 + 2, 4) * quad, HDIM), quad)]
    biggest(1)
    settle(0)
    own_beside(0)

    for by in range(1, 16):
        mx_copy(1, by).start()

    def units(group, t, first, last):
        for l in range(first, last):
            unit(group, t, l)

    work = {15: (0, 0, 0, 4), 16: (0, 1, 0, 4), 17: (0, 2, 0, 4), 18: (0, 3, 0, 4)}
    work.update({21: (1, 0, 0, 4), 22: (1, 1, 0, 4), 24: (1, 2, 0, 2), 26: (1, 2, 2, 4)})
    work.update({27: (1, 3, 0, 2), 28: (1, 3, 2, 4)})
    for slot in range(15, 29):
        beside(slot - 1)
        if slot < 28:
            ring(slot)
        if slot == 21:
            settle(1)
            own_beside(1)
        if slot in work:
            units(*work[slot])

    total(g_ref.at[pl.ds(0, 7), 0], z_send, z_recv.at[0]).wait_send()
    total(g_ref.at[pl.ds(0, 8), 0], d_send, z_recv.at[0]).wait_send()
    total(g_ref.at[pl.ds(0, 7), 0, pl.ds(0, 4)], xy_send, z_recv.at[0]).wait_send()
    total(mx_ref.at[pl.ds(0, 2), pl.ds(1, 15)], mx_send, mx_recv.at[0]).wait_send()


def piece(l, c):
    if c < 2:
        return 2 * (1 - c) + l // 2, l % 2
    return 4 + l, c - 2


def output_kernel(
    src_ref, tgt_ref, c_ref, acc_ref, pk_ref, last_ref,
    codes_hbm, peaks_ref, checked_hbm,
    chk_ref, sem, chk_sem,
):
    col = lax.axis_index("col")
    z = lax.axis_index("row") // 2
    quad = c_ref.shape[2] // 4
    classes = recv_classes(src_ref, tgt_ref, col)
    slots = []
    for c in range(4):
        at = jnp.int32(0)
        for j in range(1, PER):
            at = jnp.where(classes[j] == c, j, at)
        slots.append(at)

    def lanes(c):
        return pl.ds(pl.multiple_of(slots[c] * HDIM, HDIM), HDIM)

    copies = []
    for l in range(LAYERS):
        for c in range(4):
            copy = pltpu.make_async_copy(
                c_ref.at[piece(l, c)], codes_hbm.at[l, :, lanes(c)], sem.at[l, c]
            )
            copy.start()
            copies.append(copy)
    start = pl.multiple_of(rem(z // 2 + 2, 4) * quad, HDIM)

    def put(l, c, block):
        q, half = piece(l, c)
        scale = pk_ref[q // 4, half * 4 + q % 4:half * 4 + q % 4 + 1, :]
        chk_ref[l, c] = (block * scale).astype(jnp.bfloat16)
        copy = pltpu.make_async_copy(
            chk_ref.at[l, c], checked_hbm.at[l, :, lanes(c)], chk_sem.at[l, c]
        )
        copy.start()
        copies.append(copy)

    for l in range(LAYERS):
        for c in range(2):
            q, half = piece(l, c)
            put(l, c, acc_ref[q, :, half * HDIM:(half + 1) * HDIM])
    for l in range(LAYERS):
        both = jnp.concatenate(
            [c_ref[4 + l, 0, pl.ds(start, quad), :], c_ref[4 + l, 1, pl.ds(start, quad), :]], axis=1
        )
        last = acc_ref[4 + l] + jnp.dot(
            last_ref[...], both, preferred_element_type=jnp.float32
        )
        for c in range(2, 4):
            put(l, c, last[:, (c - 2) * HDIM:(c - 1) * HDIM])
    lane = lax.broadcasted_iota(jnp.int32, (LAYERS, HDIM), 1)
    out = jnp.zeros((LAYERS, HDIM), jnp.float32)
    for c in range(4):
        rows = []
        for l in range(LAYERS):
            q, half = piece(l, c)
            rows.append(pk_ref[q // 4, half * 4 + q % 4:half * 4 + q % 4 + 1, :])
        out = jnp.where(lane == slots[c], jnp.concatenate(rows, axis=0), out)
    peaks_ref[...] = out[:, :PER]
    for copy in copies:
        copy.wait()


def per_device(train_weight, src_map, tgt_map, probe):
    layers, depth, width = train_weight.shape
    tokens, model = probe.shape
    bf16, f32 = jnp.bfloat16, jnp.float32
    smem = pl.BlockSpec(memory_space=pltpu.SMEM)
    vmem = pl.BlockSpec(memory_space=pltpu.VMEM)
    hbm = pl.BlockSpec(memory_space=pl.ANY)
    three = pltpu.VMEM((3, 2, depth, HDIM), bf16)
    two = pltpu.VMEM((2, 2, depth, HDIM), bf16)
    dma = pltpu.SemaphoreType.DMA
    c, acc, pk, held = pl.pallas_call(
        gather_kernel,
        name="gather_codes",
        out_shape=(
            pltpu.VMEM((8, 2, model, HDIM), bf16),
            pltpu.VMEM((8, tokens, 2 * HDIM), f32),
            pltpu.VMEM((2, 8, HDIM), f32),
            pltpu.VMEM((tokens, model // 4), bf16),
        ),
        in_specs=[smem, smem, hbm, hbm],
        out_specs=(vmem, vmem, vmem, vmem),
        scratch_shapes=[
            pltpu.VMEM((NZ, 2, 8, 2, depth, HDIM), bf16),
            pltpu.VMEM((tokens, model), bf16),
            pltpu.VMEM((layers, depth, width), bf16),
            pltpu.VMEM((layers, 2, depth, HDIM), bf16),
            pltpu.VMEM((2, 16, 8, HDIM), f32),
            pltpu.VMEM((2, 8, HDIM), f32),
            pltpu.VMEM((2, 8, HDIM), f32),
        ]
        + [three] * 4 + [two] * 4 + [three] * 4 + [two] * 4
        + [
            dma((4,)), dma, dma((4, 2)), dma((4, 4)), dma((28,)), dma((2,)), dma((28,)), dma((2,)),
            dma, dma, dma, dma,
        ],
        compiler_params=pltpu.CompilerParams(
            collective_id=0, has_side_effects=True, vmem_limit_bytes=34 * 1024 * 1024
        ),
    )(src_map, tgt_map, train_weight, probe)
    return pl.pallas_call(
        output_kernel,
        name="write_outputs",
        out_shape=(
            jax.ShapeDtypeStruct((layers, model, width), bf16),
            jax.ShapeDtypeStruct((layers, PER), f32),
            jax.ShapeDtypeStruct((layers, tokens, width), bf16),
        ),
        in_specs=[smem, smem, vmem, vmem, vmem, vmem],
        out_specs=(hbm, vmem, hbm),
        scratch_shapes=[
            pltpu.VMEM((layers, 4, tokens, HDIM), bf16),
            dma((4, 4)),
            dma((4, 4)),
        ],
        compiler_params=pltpu.CompilerParams(vmem_limit_bytes=4 * 1024 * 1024),
    )(src_map, tgt_map, c, acc, pk, held)


def solution(mesh):
    in_specs = (P(None, "row", "col"), P(), P(), P("row", None))
    out_specs = (P(None, None, "col"), P(None, "col"), P(None, "row", "col"))
    return jax.shard_map(
        per_device, mesh=mesh, in_specs=in_specs, out_specs=out_specs, check_vma=False
    )
```

```python
import functools

import jax
import jax.numpy as jnp
from jax import lax
from jax.experimental import pallas as pl
from jax.experimental.pallas import tpu as pltpu
from jax.sharding import PartitionSpec as P

HDIM = 128
MESH = pl.DeviceIdType.MESH
LAYERS = 4
NZ = 8
NCOL = 16
HEADS = 64
PER = 4
EPS = 1e-06


def rem(a, n):
    return lax.rem(a, n)


def send_classes(src_ref, tgt_ref, col):
    heads = [src_ref[col * PER + i] for i in range(PER)]

    def look(t, found):
        head = tgt_ref[t]
        return tuple(jnp.where(head == h, t, f) for h, f in zip(heads, found))

    zero = jnp.int32(0)
    found = lax.fori_loop(0, HEADS, look, (zero,) * PER, unroll=8)
    shifts = [rem(f // PER - col + NCOL, NCOL) for f in found]

    def first(test):
        at = jnp.int32(PER - 1)
        for i in range(PER - 2, -1, -1):
            at = jnp.where(test(shifts[i]), i, at)
        return at

    at_a = first(lambda s: s == 8)
    at_b = first(lambda s: s == 1)
    at_s = first(lambda s: (s != 8) & (s != 1))
    at_e = 6 - at_a - at_b - at_s

    def pick(at):
        value = shifts[PER - 1]
        for i in range(PER - 2, -1, -1):
            value = jnp.where(at == i, shifts[i], value)
        return value

    return at_a, at_b, at_s, at_e, pick(at_s), pick(at_e)


def recv_classes(src_ref, tgt_ref, col):
    wanted = [tgt_ref[col * PER + j] for j in range(PER)]

    def look(t, found):
        head = src_ref[t]
        return tuple(jnp.where(head == h, t, f) for h, f in zip(wanted, found))

    zero = jnp.int32(0)
    found = lax.fori_loop(0, HEADS, look, (zero,) * PER, unroll=8)
    classes = []
    for f in found:
        from_col = f // PER
        place = rem(f, PER)
        shift = rem(col - from_col + NCOL, NCOL)
        later = jnp.int32(0)
        for i in range(PER - 1):
            head = src_ref[from_col * PER + i]
            mine = jnp.int32(0)
            for h in wanted:
                mine = jnp.where(head == h, 1, mine)
            later = jnp.where(i < place, jnp.maximum(later, mine), later)
        kind = jnp.where(shift == 8, 0, jnp.where(shift == 1, 1, 2))
        classes.append(jnp.where(later == 1, 3, kind))
    return classes


def gather_kernel(
    src_ref, tgt_ref, w_hbm, probe_hbm,
    c_ref, acc_ref, pk_ref, last_ref,
    g_ref, probe_ref, w_ref, sb_ref, mx_ref, mine_ref, rk_ref,
    x1a, x1b, x1c, x1d, x2a, x2b, x2c, x2d,
    y1a, y1b, y1c, y1d, y2a, y2b, y2c, y2d,
    w_sem, p_sem, ab_recv, xy_recv, z_recv, own_recv, d_recv, mx_recv,
    xy_send, z_send, d_send, mx_send,
):
    x1, x2 = (x1a, x1b, x1c, x1d), (x2a, x2b, x2c, x2d)
    y1, y2 = (y1a, y1b, y1c, y1d), (y2a, y2b, y2c, y2d)
    row = lax.axis_index("row")
    col = lax.axis_index("col")
    z, core = row // 2, rem(row, 2)
    depth = w_ref.shape[1]
    quad = 4 * depth

    def w_copy(l):
        return pltpu.make_async_copy(w_hbm.at[l], w_ref.at[l], w_sem.at[l])

    def p_copy():
        return pltpu.make_async_copy(probe_hbm, probe_ref, p_sem)

    barrier = pltpu.get_barrier_semaphore()
    for d in range(1, 16):
        pl.semaphore_signal(barrier, inc=1, device_id=(rem(row + d, 16), col), device_id_type=MESH)
    y = rem(col, 4)
    x_next, x_back = rem(col + 4, NCOL), rem(col + 12, NCOL)
    y_next, y_back = col - y + rem(y + 1, 4), col - y + rem(y + 3, 4)
    for to in (rem(col + 8, NCOL), rem(col + 1, NCOL), rem(col + 15, NCOL), x_next, x_back, y_next, y_back):
        pl.semaphore_signal(barrier, inc=1, device_id=(row, to), device_id_type=MESH)
    for l in range(LAYERS):
        w_copy(l).start()
    p_copy().start()

    at_a, at_b, at_s, at_e, s_by, e_by = send_classes(src_ref, tgt_ref, col)
    s_y, e_y = rem(s_by, 4), rem(e_by, 4)
    s_x = rem(s_by // 4 + jnp.where(y < s_y, 1, 0), 4)
    e_x = rem(e_by // 4 + jnp.where(y < e_y, 1, 0), 4)

    def steps(s_part, e_part):
        first_s = jnp.where(s_part == 0, 0, jnp.where(s_part == 3, 2, 1))
        first_e = jnp.where(e_part == 0, 0, jnp.where(e_part == 1, 1, 2))
        return first_s, first_e, jnp.where(s_part == 2, 1, 0), jnp.where(e_part == 2, 1, 0)

    y1_s, y1_e, y2_s, y2_e = steps(s_y, e_y)
    x1_s, x1_e, x2_s, x2_e = steps(s_x, e_x)

    def choose(at, values):
        out = values[-1]
        for i in range(len(values) - 2, -1, -1):
            out = jnp.where(at == i, values[i], out)
        return out

    def head(l, at):
        return choose(at, [w_ref[l, :, i * HDIM:(i + 1) * HDIM] for i in range(PER)])

    for l in range(LAYERS):
        w_copy(l).wait()
        sb_ref[l, 0] = head(l, at_a)
        sb_ref[l, 1] = head(l, at_b)
        y1[l][0, 0] = head(l, at_s)
        y1[l][0, 1] = head(l, at_e)

    @pl.loop(0, 8)
    def _(q):
        acc_ref[q] = jnp.zeros(acc_ref.shape[1:], jnp.float32)

    pl.semaphore_wait(barrier, 22)

    def total(part, send, recv):
        return pltpu.make_async_remote_copy(
            src_ref=part, dst_ref=part, send_sem=send, recv_sem=recv,
            device_id=(row, rem(col + 1, NCOL)), device_id_type=MESH,
        )

    def to_col(src, dst, recv, to):
        return pltpu.make_async_remote_copy(
            src_ref=src, dst_ref=dst, send_sem=xy_send, recv_sem=recv,
            device_id=(row, to), device_id_type=MESH,
        )

    def a_copy(l):
        return to_col(sb_ref.at[l, 0], g_ref.at[0, 0, 2 + l // 2, l % 2], ab_recv.at[l, 0], rem(col + 8, NCOL))

    def b_copy(l):
        return to_col(sb_ref.at[l, 1], g_ref.at[0, 0, l // 2, l % 2], ab_recv.at[l, 1], rem(col + 1, NCOL))

    def wide_copy(stage, buffer, l, way, to):
        return to_col(buffer[l].at[0], buffer[l].at[1 + way], xy_recv.at[stage, l], to[way])

    def half_copy(stage, buffer, l, half, to):
        return to_col(buffer[l].at[0, half], buffer[l].at[1, half], xy_recv.at[stage, l], to[half])

    def shifted(stage, buffer, l):
        part = buffer[l].at[pl.ds(0, 2)] if stage % 2 == 0 else buffer[l].at[0]
        total(part, xy_send, xy_recv.at[stage, l]).wait_recv()

    for l in range(LAYERS):
        b_copy(l).start()
        a_copy(l).start()
    for l in range(LAYERS):
        for way in range(2):
            wide_copy(0, y1, l, way, (y_next, y_back)).start()

    def z_copy(way, d, at, slot):
        to = rem(z + (1, NZ - 1)[way], NZ) * 2 + core
        return pltpu.make_async_remote_copy(
            src_ref=g_ref.at[(d, 0) + at], dst_ref=g_ref.at[((d + (NZ - 1, 1)[way]) % NZ, 0) + at],
            send_sem=z_send, recv_sem=z_recv.at[slot],
            device_id=(to, col), device_id_type=MESH,
        )

    def d_copy(d, q, recv):
        return pltpu.make_async_remote_copy(
            src_ref=g_ref.at[d, 0, q], dst_ref=g_ref.at[d, 1, q],
            send_sem=d_send, recv_sem=recv,
            device_id=(z * 2 + 1 - core, col), device_id_type=MESH,
        )

    def send_own(q, half=None):
        at = (q,) if half is None else (q, half)
        for way in range(2):
            z_copy(way, 0, at, q // 4 * 14 + q % 4).start()
        if half != 0:
            d_copy(0, q, own_recv.at[q // 4]).start()

    def own_beside(group):
        total(g_ref.at[0, 0, pl.ds(0, 4)], d_send, own_recv.at[group]).wait_recv()

    def place(way, slot):
        group, i = slot // 14, slot % 14
        hop = i // 4 + 1
        q = group * 4 + (i % 4 if i < 12 else 2 * (i - 12) + way)
        return (NZ - hop, hop)[way], q

    def ring(slot):
        i = slot % 14
        total(g_ref.at[0, 0, pl.ds(0, 2)], z_send, z_recv.at[slot]).wait_recv()
        for way in range(2):
            d, q = place(way, slot)
            if i < 8:
                z_copy(way, d, (q,), slot + 4).start()
            elif i < 12 and i % 2 == way:
                z_copy(way, d, (q,), slot - i + 12 + (i - 8) // 2).start()
        for way in range(2):
            d, q = place(way, slot)
            d_copy(d, q, d_recv.at[slot]).start()

    def beside(slot):
        total(g_ref.at[0, 0, pl.ds(0, 2)], d_send, d_recv.at[slot]).wait_recv()

    def biggest(group):
        rows = []
        for half in range(2):
            for l in range(LAYERS):
                block = g_ref[0, 0, group * 4 + l, half]
                rows.append(jnp.max(jnp.abs(block.astype(jnp.float32)), axis=0, keepdims=True))
        mine_ref[group] = jnp.concatenate(rows, axis=0)

    def mx_copy(group, by):
        return pltpu.make_async_remote_copy(
            src_ref=mine_ref.at[group], dst_ref=mx_ref.at[group, by],
            send_sem=mx_send, recv_sem=mx_recv.at[group],
            device_id=(rem(row + by, 16), col), device_id_type=MESH,
        )

    def settle(group):
        total(mx_ref.at[group, pl.ds(1, 15)], mx_send, mx_recv.at[group]).wait_recv()
        top = mine_ref[group]
        for rb in range(1, 16):
            top = jnp.maximum(top, mx_ref[group, rb])
        top = jnp.broadcast_to(jnp.max(top, axis=1, keepdims=True), top.shape)
        pk_ref[group] = top
        rk_ref[group] = 1.0 / ((top + EPS) * 0.0625)

    even = rem(z, 2) == 0

    def unit(group, t, l):
        p = rem(z // 2 + (0, -1, 1, 2)[t] * (1 - 2 * rem(z, 2)) + 4, 4)
        q = group * 4 + l
        start = pl.multiple_of(p * quad, HDIM)
        for half in range(2):
            scale = rk_ref[group, half * 4 + l:half * 4 + l + 1, :]
            for d in ((0, 1), (-1, -2), (2, 3), (-3, 4))[t]:
                for other in range(2):
                    block = g_ref[d % NZ, other, q, half]
                    if d % 4:
                        block = jnp.where(even, block, g_ref[-d % NZ, other, q, half])
                    at = start + rem(z + d + NZ, 2) * (2 * depth) + (core + other - 2 * core * other) * depth
                    c_ref[q, half, pl.ds(pl.multiple_of(at, 16), depth), :] = (
                        (block.astype(jnp.float32) * 0.0625) * scale
                    ).astype(jnp.bfloat16)
        if group == 1 and t == 3:
            return
        both = jnp.concatenate(
            [c_ref[q, 0, pl.ds(start, quad), :], c_ref[q, 1, pl.ds(start, quad), :]], axis=1
        )
        acc_ref[q] += jnp.dot(
            probe_ref[:, pl.ds(start, quad)], both, preferred_element_type=jnp.float32
        )

    def took(kind, l):
        (a_copy, b_copy)[kind](l).wait_recv()
        send_own(2 * (1 - kind) + l // 2, l % 2)

    took(1, 0)
    took(1, 1)
    took(0, 0)
    took(1, 2)
    took(1, 3)
    took(0, 1)
    ring(0)
    took(0, 2)
    beside(0)
    ring(1)
    took(0, 3)
    biggest(0)

    for i in range(2, 15):
        if i == 3:
            for by in range(1, 16):
                mx_copy(0, by).start()
        sends = []
        l = i - 4
        if 0 <= l < 4:
            shifted(0, y1, l)
            y2[l][0, 0] = choose(y1_s, [y1[l][k, 0] for k in range(3)])
            y2[l][0, 1] = choose(y1_e, [y1[l][k, 1] for k in range(3)])
            sends += [half_copy(1, y2, l, half, (y_next, y_back)) for half in range(2)]
        l = i - 7
        if 0 <= l < 4:
            shifted(1, y2, l)
            x1[l][0, 0] = choose(y2_s, [y2[l][k, 0] for k in range(2)])
            x1[l][0, 1] = choose(y2_e, [y2[l][k, 1] for k in range(2)])
            sends += [wide_copy(2, x1, l, way, (x_next, x_back)) for way in range(2)]
        l = i - 9
        if 0 <= l < 4:
            shifted(2, x1, l)
            x2[l][0, 0] = choose(x1_s, [x1[l][k, 0] for k in range(3)])
            x2[l][0, 1] = choose(x1_e, [x1[l][k, 1] for k in range(3)])
            sends += [half_copy(3, x2, l, half, (x_next, x_back)) for half in range(2)]
        l = i - 11
        own = None
        if 0 <= l < 4:
            shifted(3, x2, l)
            g_ref[0, 0, 4 + l, 0] = choose(x2_s, [x2[l][k, 0] for k in range(2)])
            g_ref[0, 0, 4 + l, 1] = choose(x2_e, [x2[l][k, 1] for k in range(2)])
            own = 4 + l
        beside(i - 1)
        for copy in sends:
            copy.start()
        if own is not None:
            send_own(own)
        ring(i)

    p_copy().wait()
    last_ref[...] = probe_ref[:, pl.ds(pl.multiple_of(rem(z // 2 + 2, 4) * quad, HDIM), quad)]
    biggest(1)
    settle(0)
    own_beside(0)

    for by in range(1, 16):
        mx_copy(1, by).start()

    def units(group, t, first, last):
        for l in range(first, last):
            unit(group, t, l)

    work = {15: (0, 0, 0, 4), 16: (0, 1, 0, 4), 17: (0, 2, 0, 4), 18: (0, 3, 0, 4)}
    work.update({21: (1, 0, 0, 4), 22: (1, 1, 0, 4), 24: (1, 2, 0, 2), 26: (1, 2, 2, 4)})
    work.update({27: (1, 3, 0, 2), 28: (1, 3, 2, 4)})
    for slot in range(15, 29):
        beside(slot - 1)
        if slot < 28:
            ring(slot)
        if slot == 21:
            settle(1)
            own_beside(1)
        if slot in work:
            units(*work[slot])

    total(g_ref.at[pl.ds(0, 7), 0], z_send, z_recv.at[0]).wait_send()
    total(g_ref.at[pl.ds(0, 8), 0], d_send, z_recv.at[0]).wait_send()
    total(g_ref.at[pl.ds(0, 7), 0, pl.ds(0, 4)], xy_send, z_recv.at[0]).wait_send()
    total(mx_ref.at[pl.ds(0, 2), pl.ds(1, 15)], mx_send, mx_recv.at[0]).wait_send()


def piece(l, c):
    if c < 2:
        return 2 * (1 - c) + l // 2, l % 2
    return 4 + l, c - 2


def output_kernel(
    src_ref, tgt_ref, c_ref, acc_ref, pk_ref, last_ref,
    codes_hbm, peaks_ref, checked_hbm,
    chk_ref, sem, chk_sem,
):
    col = lax.axis_index("col")
    z = lax.axis_index("row") // 2
    quad = c_ref.shape[2] // 4
    classes = recv_classes(src_ref, tgt_ref, col)
    slots = []
    for c in range(4):
        at = jnp.int32(0)
        for j in range(1, PER):
            at = jnp.where(classes[j] == c, j, at)
        slots.append(at)

    def lanes(c):
        return pl.ds(pl.multiple_of(slots[c] * HDIM, HDIM), HDIM)

    copies = []
    for l in range(LAYERS):
        for c in range(4):
            copy = pltpu.make_async_copy(
                c_ref.at[piece(l, c)], codes_hbm.at[l, :, lanes(c)], sem.at[l, c]
            )
            copy.start()
            copies.append(copy)
    start = pl.multiple_of(rem(z // 2 + 2, 4) * quad, HDIM)

    def put(l, c, block):
        q, half = piece(l, c)
        scale = pk_ref[q // 4, half * 4 + q % 4:half * 4 + q % 4 + 1, :]
        chk_ref[l, c] = (block * scale).astype(jnp.bfloat16)
        copy = pltpu.make_async_copy(
            chk_ref.at[l, c], checked_hbm.at[l, :, lanes(c)], chk_sem.at[l, c]
        )
        copy.start()
        copies.append(copy)

    for l in range(LAYERS):
        for c in range(2):
            q, half = piece(l, c)
            put(l, c, acc_ref[q, :, half * HDIM:(half + 1) * HDIM])
    for l in range(LAYERS):
        both = jnp.concatenate(
            [c_ref[4 + l, 0, pl.ds(start, quad), :], c_ref[4 + l, 1, pl.ds(start, quad), :]], axis=1
        )
        last = acc_ref[4 + l] + jnp.dot(
            last_ref[...], both, preferred_element_type=jnp.float32
        )
        for c in range(2, 4):
            put(l, c, last[:, (c - 2) * HDIM:(c - 1) * HDIM])
    lane = lax.broadcasted_iota(jnp.int32, (LAYERS, HDIM), 1)
    out = jnp.zeros((LAYERS, HDIM), jnp.float32)
    for c in range(4):
        rows = []
        for l in range(LAYERS):
            q, half = piece(l, c)
            rows.append(pk_ref[q // 4, half * 4 + q % 4:half * 4 + q % 4 + 1, :])
        out = jnp.where(lane == slots[c], jnp.concatenate(rows, axis=0), out)
    peaks_ref[...] = out[:, :PER]
    for copy in copies:
        copy.wait()


def per_device(train_weight, src_map, tgt_map, probe):
    layers, depth, width = train_weight.shape
    tokens, model = probe.shape
    bf16, f32 = jnp.bfloat16, jnp.float32
    smem = pl.BlockSpec(memory_space=pltpu.SMEM)
    vmem = pl.BlockSpec(memory_space=pltpu.VMEM)
    hbm = pl.BlockSpec(memory_space=pl.ANY)
    three = pltpu.VMEM((3, 2, depth, HDIM), bf16)
    two = pltpu.VMEM((2, 2, depth, HDIM), bf16)
    dma = pltpu.SemaphoreType.DMA
    c, acc, pk, held = pl.pallas_call(
        gather_kernel,
        name="gather_codes",
        out_shape=(
            pltpu.VMEM((8, 2, model, HDIM), bf16),
            pltpu.VMEM((8, tokens, 2 * HDIM), f32),
            pltpu.VMEM((2, 8, HDIM), f32),
            pltpu.VMEM((tokens, model // 4), bf16),
        ),
        in_specs=[smem, smem, hbm, hbm],
        out_specs=(vmem, vmem, vmem, vmem),
        scratch_shapes=[
            pltpu.VMEM((NZ, 2, 8, 2, depth, HDIM), bf16),
            pltpu.VMEM((tokens, model), bf16),
            pltpu.VMEM((layers, depth, width), bf16),
            pltpu.VMEM((layers, 2, depth, HDIM), bf16),
            pltpu.VMEM((2, 16, 8, HDIM), f32),
            pltpu.VMEM((2, 8, HDIM), f32),
            pltpu.VMEM((2, 8, HDIM), f32),
        ]
        + [three] * 4 + [two] * 4 + [three] * 4 + [two] * 4
        + [
            dma((4,)), dma, dma((4, 2)), dma((4, 4)), dma((28,)), dma((2,)), dma((28,)), dma((2,)),
            dma, dma, dma, dma,
        ],
        compiler_params=pltpu.CompilerParams(
            collective_id=0, has_side_effects=True, vmem_limit_bytes=34 * 1024 * 1024
        ),
    )(src_map, tgt_map, train_weight, probe)
    return pl.pallas_call(
        output_kernel,
        name="write_outputs",
        out_shape=(
            jax.ShapeDtypeStruct((layers, model, width), bf16),
            jax.ShapeDtypeStruct((layers, PER), f32),
            jax.ShapeDtypeStruct((layers, tokens, width), bf16),
        ),
        in_specs=[smem, smem, vmem, vmem, vmem, vmem],
        out_specs=(hbm, vmem, hbm),
        scratch_shapes=[
            pltpu.VMEM((layers, 4, tokens, HDIM), bf16),
            dma((4, 4)),
            dma((4, 4)),
        ],
        compiler_params=pltpu.CompilerParams(vmem_limit_bytes=4 * 1024 * 1024),
    )(src_map, tgt_map, c, acc, pk, held)


def solution(mesh):
    in_specs = (P(None, "row", "col"), P(), P(), P("row", None))
    out_specs = (P(None, None, "col"), P(None, "col"), P(None, "row", "col"))
    return jax.shard_map(
        per_device, mesh=mesh, in_specs=in_specs, out_specs=out_specs, check_vma=False
    )
```

```python
import functools

import jax
import jax.numpy as jnp
from jax import lax
from jax.experimental import pallas as pl
from jax.experimental.pallas import tpu as pltpu
from jax.sharding import PartitionSpec as P

HDIM = 128
MESH = pl.DeviceIdType.MESH
LAYERS = 4
NZ = 8
NCOL = 16
HEADS = 64
PER = 4
EPS = 1e-06


def rem(a, n):
    return lax.rem(a, n)


def send_classes(src_ref, tgt_ref, col):
    heads = [src_ref[col * PER + i] for i in range(PER)]

    def look(t, found):
        head = tgt_ref[t]
        return tuple(jnp.where(head == h, t, f) for h, f in zip(heads, found))

    zero = jnp.int32(0)
    found = lax.fori_loop(0, HEADS, look, (zero,) * PER, unroll=8)
    shifts = [rem(f // PER - col + NCOL, NCOL) for f in found]

    def first(test):
        at = jnp.int32(PER - 1)
        for i in range(PER - 2, -1, -1):
            at = jnp.where(test(shifts[i]), i, at)
        return at

    at_a = first(lambda s: s == 8)
    at_b = first(lambda s: s == 1)
    at_s = first(lambda s: (s != 8) & (s != 1))
    at_e = 6 - at_a - at_b - at_s

    def pick(at):
        value = shifts[PER - 1]
        for i in range(PER - 2, -1, -1):
            value = jnp.where(at == i, shifts[i], value)
        return value

    return at_a, at_b, at_s, at_e, pick(at_s), pick(at_e)


def recv_classes(src_ref, tgt_ref, col):
    wanted = [tgt_ref[col * PER + j] for j in range(PER)]

    def look(t, found):
        head = src_ref[t]
        return tuple(jnp.where(head == h, t, f) for h, f in zip(wanted, found))

    zero = jnp.int32(0)
    found = lax.fori_loop(0, HEADS, look, (zero,) * PER, unroll=8)
    classes = []
    for f in found:
        from_col = f // PER
        place = rem(f, PER)
        shift = rem(col - from_col + NCOL, NCOL)
        later = jnp.int32(0)
        for i in range(PER - 1):
            head = src_ref[from_col * PER + i]
            mine = jnp.int32(0)
            for h in wanted:
                mine = jnp.where(head == h, 1, mine)
            later = jnp.where(i < place, jnp.maximum(later, mine), later)
        kind = jnp.where(shift == 8, 0, jnp.where(shift == 1, 1, 2))
        classes.append(jnp.where(later == 1, 3, kind))
    return classes


def gather_kernel(
    src_ref, tgt_ref, w_hbm, probe_hbm,
    c_ref, acc_ref, pk_ref, last_ref,
    g_ref, probe_ref, w_ref, sb_ref, mx_ref, mine_ref, rk_ref,
    x1a, x1b, x1c, x1d, x2a, x2b, x2c, x2d,
    y1a, y1b, y1c, y1d, y2a, y2b, y2c, y2d,
    w_sem, p_sem, ab_recv, xy_recv, z_recv, own_recv, d_recv, mx_recv,
    xy_send, z_send, d_send, mx_send,
):
    x1, x2 = (x1a, x1b, x1c, x1d), (x2a, x2b, x2c, x2d)
    y1, y2 = (y1a, y1b, y1c, y1d), (y2a, y2b, y2c, y2d)
    row = lax.axis_index("row")
    col = lax.axis_index("col")
    z, core = row // 2, rem(row, 2)
    depth = w_ref.shape[1]
    quad = 4 * depth

    def w_copy(l):
        return pltpu.make_async_copy(w_hbm.at[l], w_ref.at[l], w_sem.at[l])

    def p_copy():
        return pltpu.make_async_copy(probe_hbm, probe_ref, p_sem)

    barrier = pltpu.get_barrier_semaphore()
    for d in range(1, 16):
        pl.semaphore_signal(barrier, inc=1, device_id=(rem(row + d, 16), col), device_id_type=MESH)
    y = rem(col, 4)
    x_next, x_back = rem(col + 4, NCOL), rem(col + 12, NCOL)
    y_next, y_back = col - y + rem(y + 1, 4), col - y + rem(y + 3, 4)
    for to in (rem(col + 8, NCOL), rem(col + 1, NCOL), rem(col + 15, NCOL), x_next, x_back, y_next, y_back):
        pl.semaphore_signal(barrier, inc=1, device_id=(row, to), device_id_type=MESH)
    for l in range(LAYERS):
        w_copy(l).start()
    p_copy().start()

    at_a, at_b, at_s, at_e, s_by, e_by = send_classes(src_ref, tgt_ref, col)
    s_y, e_y = rem(s_by, 4), rem(e_by, 4)
    s_x = rem(s_by // 4 + jnp.where(y < s_y, 1, 0), 4)
    e_x = rem(e_by // 4 + jnp.where(y < e_y, 1, 0), 4)

    def steps(s_part, e_part):
        first_s = jnp.where(s_part == 0, 0, jnp.where(s_part == 3, 2, 1))
        first_e = jnp.where(e_part == 0, 0, jnp.where(e_part == 1, 1, 2))
        return first_s, first_e, jnp.where(s_part == 2, 1, 0), jnp.where(e_part == 2, 1, 0)

    y1_s, y1_e, y2_s, y2_e = steps(s_y, e_y)
    x1_s, x1_e, x2_s, x2_e = steps(s_x, e_x)

    def choose(at, values):
        out = values[-1]
        for i in range(len(values) - 2, -1, -1):
            out = jnp.where(at == i, values[i], out)
        return out

    def head(l, at):
        return choose(at, [w_ref[l, :, i * HDIM:(i + 1) * HDIM] for i in range(PER)])

    for l in range(LAYERS):
        w_copy(l).wait()
        sb_ref[l, 0] = head(l, at_a)
        sb_ref[l, 1] = head(l, at_b)

    pl.semaphore_wait(barrier, 22)

    def total(part, send, recv):
        return pltpu.make_async_remote_copy(
            src_ref=part, dst_ref=part, send_sem=send, recv_sem=recv,
            device_id=(row, rem(col + 1, NCOL)), device_id_type=MESH,
        )

    def to_col(src, dst, recv, to):
        return pltpu.make_async_remote_copy(
            src_ref=src, dst_ref=dst, send_sem=xy_send, recv_sem=recv,
            device_id=(row, to), device_id_type=MESH,
        )

    def a_copy(l):
        return to_col(sb_ref.at[l, 0], g_ref.at[0, 0, 2 + l // 2, l % 2], ab_recv.at[l, 0], rem(col + 8, NCOL))

    def b_copy(l):
        return to_col(sb_ref.at[l, 1], g_ref.at[0, 0, l // 2, l % 2], ab_recv.at[l, 1], rem(col + 1, NCOL))

    def wide_copy(stage, buffer, l, way, to):
        return to_col(buffer[l].at[0], buffer[l].at[1 + way], xy_recv.at[stage, l], to[way])

    def half_copy(stage, buffer, l, half, to):
        return to_col(buffer[l].at[0, half], buffer[l].at[1, half], xy_recv.at[stage, l], to[half])

    def shifted(stage, buffer, l):
        part = buffer[l].at[pl.ds(0, 2)] if stage % 2 == 0 else buffer[l].at[0]
        total(part, xy_send, xy_recv.at[stage, l]).wait_recv()

    for l in range(LAYERS):
        b_copy(l).start()
        a_copy(l).start()
    for l in range(LAYERS):
        y1[l][0, 0] = head(l, at_s)
        y1[l][0, 1] = head(l, at_e)

    def z_copy(way, d, at, slot):
        to = rem(z + (1, NZ - 1)[way], NZ) * 2 + core
        return pltpu.make_async_remote_copy(
            src_ref=g_ref.at[(d, 0) + at], dst_ref=g_ref.at[((d + (NZ - 1, 1)[way]) % NZ, 0) + at],
            send_sem=z_send, recv_sem=z_recv.at[slot],
            device_id=(to, col), device_id_type=MESH,
        )

    def d_copy(d, q, recv):
        return pltpu.make_async_remote_copy(
            src_ref=g_ref.at[d, 0, q], dst_ref=g_ref.at[d, 1, q],
            send_sem=d_send, recv_sem=recv,
            device_id=(z * 2 + 1 - core, col), device_id_type=MESH,
        )

    def send_own(q, half=None):
        at = (q,) if half is None else (q, half)
        for way in range(2):
            z_copy(way, 0, at, q // 4 * 14 + q % 4).start()
        if half != 0:
            d_copy(0, q, own_recv.at[q // 4]).start()

    def own_beside(group):
        total(g_ref.at[0, 0, pl.ds(0, 4)], d_send, own_recv.at[group]).wait_recv()

    def place(way, slot):
        group, i = slot // 14, slot % 14
        hop = i // 4 + 1
        q = group * 4 + (i % 4 if i < 12 else 2 * (i - 12) + way)
        return (NZ - hop, hop)[way], q

    def ring(slot):
        i = slot % 14
        total(g_ref.at[0, 0, pl.ds(0, 2)], z_send, z_recv.at[slot]).wait_recv()
        for way in range(2):
            d, q = place(way, slot)
            if i < 8:
                z_copy(way, d, (q,), slot + 4).start()
            elif i < 12 and i % 2 == way:
                z_copy(way, d, (q,), slot - i + 12 + (i - 8) // 2).start()
        for way in range(2):
            d, q = place(way, slot)
            d_copy(d, q, d_recv.at[slot]).start()

    def beside(slot):
        total(g_ref.at[0, 0, pl.ds(0, 2)], d_send, d_recv.at[slot]).wait_recv()

    def biggest(group):
        rows = []
        for half in range(2):
            for l in range(LAYERS):
                block = g_ref[0, 0, group * 4 + l, half]
                rows.append(jnp.max(jnp.abs(block.astype(jnp.float32)), axis=0, keepdims=True))
        mine_ref[group] = jnp.concatenate(rows, axis=0)

    def mx_copy(group, by):
        return pltpu.make_async_remote_copy(
            src_ref=mine_ref.at[group], dst_ref=mx_ref.at[group, by],
            send_sem=mx_send, recv_sem=mx_recv.at[group],
            device_id=(rem(row + by, 16), col), device_id_type=MESH,
        )

    def settle(group):
        total(mx_ref.at[group, pl.ds(1, 15)], mx_send, mx_recv.at[group]).wait_recv()
        top = mine_ref[group]
        for rb in range(1, 16):
            top = jnp.maximum(top, mx_ref[group, rb])
        top = jnp.broadcast_to(jnp.max(top, axis=1, keepdims=True), top.shape)
        pk_ref[group] = top
        rk_ref[group] = 1.0 / ((top + EPS) * 0.0625)

    even = rem(z, 2) == 0

    def unit(group, t, l):
        p = rem(z // 2 + (0, -1, 1, 2)[t] * (1 - 2 * rem(z, 2)) + 4, 4)
        q = group * 4 + l
        start = pl.multiple_of(p * quad, HDIM)
        for half in range(2):
            scale = rk_ref[group, half * 4 + l:half * 4 + l + 1, :]
            for d in ((0, 1), (-1, -2), (2, 3), (-3, 4))[t]:
                for other in range(2):
                    block = g_ref[d % NZ, other, q, half]
                    if d % 4:
                        block = jnp.where(even, block, g_ref[-d % NZ, other, q, half])
                    at = start + rem(z + d + NZ, 2) * (2 * depth) + (core + other - 2 * core * other) * depth
                    c_ref[q, half, pl.ds(pl.multiple_of(at, 16), depth), :] = (
                        (block.astype(jnp.float32) * 0.0625) * scale
                    ).astype(jnp.bfloat16)
        if group == 1 and t == 3:
            return
        both = jnp.concatenate(
            [c_ref[q, 0, pl.ds(start, quad), :], c_ref[q, 1, pl.ds(start, quad), :]], axis=1
        )
        acc_ref[q] += jnp.dot(
            probe_ref[:, pl.ds(start, quad)], both, preferred_element_type=jnp.float32
        )

    def took(kind, l):
        (a_copy, b_copy)[kind](l).wait_recv()
        send_own(2 * (1 - kind) + l // 2, l % 2)

    @pl.loop(0, 8)
    def _(q):
        acc_ref[q] = jnp.zeros(acc_ref.shape[1:], jnp.float32)

    took(1, 0)
    for l in range(LAYERS):
        for way in range(2):
            wide_copy(0, y1, l, way, (y_next, y_back)).start()
    took(1, 1)
    took(0, 0)
    took(1, 2)
    took(1, 3)
    took(0, 1)
    ring(0)
    took(0, 2)
    beside(0)
    ring(1)
    took(0, 3)
    biggest(0)

    for i in range(2, 15):
        if i == 3:
            for by in range(1, 16):
                mx_copy(0, by).start()
        sends = []
        l = i - 4
        if 0 <= l < 4:
            shifted(0, y1, l)
            y2[l][0, 0] = choose(y1_s, [y1[l][k, 0] for k in range(3)])
            y2[l][0, 1] = choose(y1_e, [y1[l][k, 1] for k in range(3)])
            sends += [half_copy(1, y2, l, half, (y_next, y_back)) for half in range(2)]
        l = i - 7
        if 0 <= l < 4:
            shifted(1, y2, l)
            x1[l][0, 0] = choose(y2_s, [y2[l][k, 0] for k in range(2)])
            x1[l][0, 1] = choose(y2_e, [y2[l][k, 1] for k in range(2)])
            sends += [wide_copy(2, x1, l, way, (x_next, x_back)) for way in range(2)]
        l = i - 9
        if 0 <= l < 4:
            shifted(2, x1, l)
            x2[l][0, 0] = choose(x1_s, [x1[l][k, 0] for k in range(3)])
            x2[l][0, 1] = choose(x1_e, [x1[l][k, 1] for k in range(3)])
            sends += [half_copy(3, x2, l, half, (x_next, x_back)) for half in range(2)]
        l = i - 11
        own = None
        if 0 <= l < 4:
            shifted(3, x2, l)
            g_ref[0, 0, 4 + l, 0] = choose(x2_s, [x2[l][k, 0] for k in range(2)])
            g_ref[0, 0, 4 + l, 1] = choose(x2_e, [x2[l][k, 1] for k in range(2)])
            own = 4 + l
        beside(i - 1)
        for copy in sends:
            copy.start()
        if own is not None:
            send_own(own)
        ring(i)

    p_copy().wait()
    last_ref[...] = probe_ref[:, pl.ds(pl.multiple_of(rem(z // 2 + 2, 4) * quad, HDIM), quad)]
    biggest(1)
    settle(0)
    own_beside(0)

    for by in range(1, 16):
        mx_copy(1, by).start()

    def units(group, t, first, last):
        for l in range(first, last):
            unit(group, t, l)

    work = {15: (0, 0, 0, 4), 16: (0, 1, 0, 4), 17: (0, 2, 0, 4), 18: (0, 3, 0, 4)}
    work.update({21: (1, 0, 0, 4), 22: (1, 1, 0, 4), 24: (1, 2, 0, 2), 26: (1, 2, 2, 4)})
    work.update({27: (1, 3, 0, 2), 28: (1, 3, 2, 4)})
    for slot in range(15, 29):
        beside(slot - 1)
        if slot < 28:
            ring(slot)
        if slot == 21:
            settle(1)
            own_beside(1)
        if slot in work:
            units(*work[slot])

    total(g_ref.at[pl.ds(0, 7), 0], z_send, z_recv.at[0]).wait_send()
    total(g_ref.at[pl.ds(0, 8), 0], d_send, z_recv.at[0]).wait_send()
    total(g_ref.at[pl.ds(0, 7), 0, pl.ds(0, 4)], xy_send, z_recv.at[0]).wait_send()
    total(mx_ref.at[pl.ds(0, 2), pl.ds(1, 15)], mx_send, mx_recv.at[0]).wait_send()


def piece(l, c):
    if c < 2:
        return 2 * (1 - c) + l // 2, l % 2
    return 4 + l, c - 2


def output_kernel(
    src_ref, tgt_ref, c_ref, acc_ref, pk_ref, last_ref,
    codes_hbm, peaks_ref, checked_hbm,
    chk_ref, sem, chk_sem,
):
    col = lax.axis_index("col")
    z = lax.axis_index("row") // 2
    quad = c_ref.shape[2] // 4
    classes = recv_classes(src_ref, tgt_ref, col)
    slots = []
    for c in range(4):
        at = jnp.int32(0)
        for j in range(1, PER):
            at = jnp.where(classes[j] == c, j, at)
        slots.append(at)

    def lanes(c):
        return pl.ds(pl.multiple_of(slots[c] * HDIM, HDIM), HDIM)

    copies = []
    for l in range(LAYERS):
        for c in range(4):
            copy = pltpu.make_async_copy(
                c_ref.at[piece(l, c)], codes_hbm.at[l, :, lanes(c)], sem.at[l, c]
            )
            copy.start()
            copies.append(copy)
    start = pl.multiple_of(rem(z // 2 + 2, 4) * quad, HDIM)

    def put(l, c, block):
        q, half = piece(l, c)
        scale = pk_ref[q // 4, half * 4 + q % 4:half * 4 + q % 4 + 1, :]
        chk_ref[l, c] = (block * scale).astype(jnp.bfloat16)
        copy = pltpu.make_async_copy(
            chk_ref.at[l, c], checked_hbm.at[l, :, lanes(c)], chk_sem.at[l, c]
        )
        copy.start()
        copies.append(copy)

    for l in range(LAYERS):
        for c in range(2):
            q, half = piece(l, c)
            put(l, c, acc_ref[q, :, half * HDIM:(half + 1) * HDIM])
    for l in range(LAYERS):
        both = jnp.concatenate(
            [c_ref[4 + l, 0, pl.ds(start, quad), :], c_ref[4 + l, 1, pl.ds(start, quad), :]], axis=1
        )
        last = acc_ref[4 + l] + jnp.dot(
            last_ref[...], both, preferred_element_type=jnp.float32
        )
        for c in range(2, 4):
            put(l, c, last[:, (c - 2) * HDIM:(c - 1) * HDIM])
    lane = lax.broadcasted_iota(jnp.int32, (LAYERS, HDIM), 1)
    out = jnp.zeros((LAYERS, HDIM), jnp.float32)
    for c in range(4):
        rows = []
        for l in range(LAYERS):
            q, half = piece(l, c)
            rows.append(pk_ref[q // 4, half * 4 + q % 4:half * 4 + q % 4 + 1, :])
        out = jnp.where(lane == slots[c], jnp.concatenate(rows, axis=0), out)
    peaks_ref[...] = out[:, :PER]
    for copy in copies:
        copy.wait()


def per_device(train_weight, src_map, tgt_map, probe):
    layers, depth, width = train_weight.shape
    tokens, model = probe.shape
    bf16, f32 = jnp.bfloat16, jnp.float32
    smem = pl.BlockSpec(memory_space=pltpu.SMEM)
    vmem = pl.BlockSpec(memory_space=pltpu.VMEM)
    hbm = pl.BlockSpec(memory_space=pl.ANY)
    three = pltpu.VMEM((3, 2, depth, HDIM), bf16)
    two = pltpu.VMEM((2, 2, depth, HDIM), bf16)
    dma = pltpu.SemaphoreType.DMA
    c, acc, pk, held = pl.pallas_call(
        gather_kernel,
        name="gather_codes",
        out_shape=(
            pltpu.VMEM((8, 2, model, HDIM), bf16),
            pltpu.VMEM((8, tokens, 2 * HDIM), f32),
            pltpu.VMEM((2, 8, HDIM), f32),
            pltpu.VMEM((tokens, model // 4), bf16),
        ),
        in_specs=[smem, smem, hbm, hbm],
        out_specs=(vmem, vmem, vmem, vmem),
        scratch_shapes=[
            pltpu.VMEM((NZ, 2, 8, 2, depth, HDIM), bf16),
            pltpu.VMEM((tokens, model), bf16),
            pltpu.VMEM((layers, depth, width), bf16),
            pltpu.VMEM((layers, 2, depth, HDIM), bf16),
            pltpu.VMEM((2, 16, 8, HDIM), f32),
            pltpu.VMEM((2, 8, HDIM), f32),
            pltpu.VMEM((2, 8, HDIM), f32),
        ]
        + [three] * 4 + [two] * 4 + [three] * 4 + [two] * 4
        + [
            dma((4,)), dma, dma((4, 2)), dma((4, 4)), dma((28,)), dma((2,)), dma((28,)), dma((2,)),
            dma, dma, dma, dma,
        ],
        compiler_params=pltpu.CompilerParams(
            collective_id=0, has_side_effects=True, vmem_limit_bytes=34 * 1024 * 1024
        ),
    )(src_map, tgt_map, train_weight, probe)
    return pl.pallas_call(
        output_kernel,
        name="write_outputs",
        out_shape=(
            jax.ShapeDtypeStruct((layers, model, width), bf16),
            jax.ShapeDtypeStruct((layers, PER), f32),
            jax.ShapeDtypeStruct((layers, tokens, width), bf16),
        ),
        in_specs=[smem, smem, vmem, vmem, vmem, vmem],
        out_specs=(hbm, vmem, hbm),
        scratch_shapes=[
            pltpu.VMEM((layers, 4, tokens, HDIM), bf16),
            dma((4, 4)),
            dma((4, 4)),
        ],
        compiler_params=pltpu.CompilerParams(vmem_limit_bytes=4 * 1024 * 1024),
    )(src_map, tgt_map, c, acc, pk, held)


def solution(mesh):
    in_specs = (P(None, "row", "col"), P(), P(), P("row", None))
    out_specs = (P(None, None, "col"), P(None, "col"), P(None, "row", "col"))
    return jax.shard_map(
        per_device, mesh=mesh, in_specs=in_specs, out_specs=out_specs, check_vma=False
    )
```

```python
import functools

import jax
import jax.numpy as jnp
from jax import lax
from jax.experimental import pallas as pl
from jax.experimental.pallas import tpu as pltpu
from jax.sharding import PartitionSpec as P

HDIM = 128
MESH = pl.DeviceIdType.MESH
LAYERS = 4
NZ = 8
NCOL = 16
HEADS = 64
PER = 4
EPS = 1e-06


def rem(a, n):
    return lax.rem(a, n)


def send_classes(src_ref, tgt_ref, col):
    heads = [src_ref[col * PER + i] for i in range(PER)]

    def look(t, found):
        head = tgt_ref[t]
        return tuple(jnp.where(head == h, t, f) for h, f in zip(heads, found))

    zero = jnp.int32(0)
    found = lax.fori_loop(0, HEADS, look, (zero,) * PER, unroll=8)
    shifts = [rem(f // PER - col + NCOL, NCOL) for f in found]

    def first(test):
        at = jnp.int32(PER - 1)
        for i in range(PER - 2, -1, -1):
            at = jnp.where(test(shifts[i]), i, at)
        return at

    at_a = first(lambda s: s == 8)
    at_b = first(lambda s: s == 1)
    at_s = first(lambda s: (s != 8) & (s != 1))
    at_e = 6 - at_a - at_b - at_s

    def pick(at):
        value = shifts[PER - 1]
        for i in range(PER - 2, -1, -1):
            value = jnp.where(at == i, shifts[i], value)
        return value

    return at_a, at_b, at_s, at_e, pick(at_s), pick(at_e)


def recv_classes(src_ref, tgt_ref, col):
    wanted = [tgt_ref[col * PER + j] for j in range(PER)]

    def look(t, found):
        head = src_ref[t]
        return tuple(jnp.where(head == h, t, f) for h, f in zip(wanted, found))

    zero = jnp.int32(0)
    found = lax.fori_loop(0, HEADS, look, (zero,) * PER, unroll=8)
    classes = []
    for f in found:
        from_col = f // PER
        place = rem(f, PER)
        shift = rem(col - from_col + NCOL, NCOL)
        later = jnp.int32(0)
        for i in range(PER - 1):
            head = src_ref[from_col * PER + i]
            mine = jnp.int32(0)
            for h in wanted:
                mine = jnp.where(head == h, 1, mine)
            later = jnp.where(i < place, jnp.maximum(later, mine), later)
        kind = jnp.where(shift == 8, 0, jnp.where(shift == 1, 1, 2))
        classes.append(jnp.where(later == 1, 3, kind))
    return classes


def gather_kernel(
    src_ref, tgt_ref, w_hbm, probe_hbm,
    c_ref, acc_ref, pk_ref, last_ref,
    g_ref, probe_ref, w_ref, sb_ref, mx_ref, mine_ref, rk_ref,
    x1a, x1b, x1c, x1d, x2a, x2b, x2c, x2d,
    y1a, y1b, y1c, y1d, y2a, y2b, y2c, y2d,
    w_sem, p_sem, ab_recv, xy_recv, z_recv, own_recv, d_recv, mx_recv,
    xy_send, z_send, d_send, mx_send,
):
    x1, x2 = (x1a, x1b, x1c, x1d), (x2a, x2b, x2c, x2d)
    y1, y2 = (y1a, y1b, y1c, y1d), (y2a, y2b, y2c, y2d)
    row = lax.axis_index("row")
    col = lax.axis_index("col")
    z, core = row // 2, rem(row, 2)
    depth = w_ref.shape[1]
    quad = 4 * depth

    def w_copy(l):
        return pltpu.make_async_copy(w_hbm.at[l], w_ref.at[l], w_sem.at[l])

    def p_copy():
        return pltpu.make_async_copy(probe_hbm, probe_ref, p_sem)

    barrier = pltpu.get_barrier_semaphore()
    for d in range(1, 16):
        pl.semaphore_signal(barrier, inc=1, device_id=(rem(row + d, 16), col), device_id_type=MESH)
    y = rem(col, 4)
    x_next, x_back = rem(col + 4, NCOL), rem(col + 12, NCOL)
    y_next, y_back = col - y + rem(y + 1, 4), col - y + rem(y + 3, 4)
    for to in (rem(col + 8, NCOL), rem(col + 1, NCOL), rem(col + 15, NCOL), x_next, x_back, y_next, y_back):
        pl.semaphore_signal(barrier, inc=1, device_id=(row, to), device_id_type=MESH)
    for l in range(LAYERS):
        w_copy(l).start()
    p_copy().start()

    at_a, at_b, at_s, at_e, s_by, e_by = send_classes(src_ref, tgt_ref, col)
    s_y, e_y = rem(s_by, 4), rem(e_by, 4)
    s_x = rem(s_by // 4 + jnp.where(y < s_y, 1, 0), 4)
    e_x = rem(e_by // 4 + jnp.where(y < e_y, 1, 0), 4)

    def steps(s_part, e_part):
        first_s = jnp.where(s_part == 0, 0, jnp.where(s_part == 3, 2, 1))
        first_e = jnp.where(e_part == 0, 0, jnp.where(e_part == 1, 1, 2))
        return first_s, first_e, jnp.where(s_part == 2, 1, 0), jnp.where(e_part == 2, 1, 0)

    y1_s, y1_e, y2_s, y2_e = steps(s_y, e_y)
    x1_s, x1_e, x2_s, x2_e = steps(s_x, e_x)

    def choose(at, values):
        out = values[-1]
        for i in range(len(values) - 2, -1, -1):
            out = jnp.where(at == i, values[i], out)
        return out

    def head(l, at):
        return choose(at, [w_ref[l, :, i * HDIM:(i + 1) * HDIM] for i in range(PER)])

    for l in range(LAYERS):
        w_copy(l).wait()
        sb_ref[l, 0] = head(l, at_a)
        sb_ref[l, 1] = head(l, at_b)
        y1[l][0, 0] = head(l, at_s)
        y1[l][0, 1] = head(l, at_e)

    @pl.loop(0, 8)
    def _(q):
        acc_ref[q] = jnp.zeros(acc_ref.shape[1:], jnp.float32)

    pl.semaphore_wait(barrier, 22)

    def total(part, send, recv):
        return pltpu.make_async_remote_copy(
            src_ref=part, dst_ref=part, send_sem=send, recv_sem=recv,
            device_id=(row, rem(col + 1, NCOL)), device_id_type=MESH,
        )

    def to_col(src, dst, recv, to):
        return pltpu.make_async_remote_copy(
            src_ref=src, dst_ref=dst, send_sem=xy_send, recv_sem=recv,
            device_id=(row, to), device_id_type=MESH,
        )

    def a_copy(l):
        return to_col(sb_ref.at[l, 0], g_ref.at[0, 0, 2 + l // 2, l % 2], ab_recv.at[l, 0], rem(col + 8, NCOL))

    def b_copy(l):
        return to_col(sb_ref.at[l, 1], g_ref.at[0, 0, l // 2, l % 2], ab_recv.at[l, 1], rem(col + 1, NCOL))

    def first_rows(part):
        return pl.ds(part * (depth // 2), depth // 2)

    def first_copy(part):
        rows = first_rows(part)
        return to_col(
            sb_ref.at[0, 1, rows], g_ref.at[0, 0, 0, 0, rows], ab_recv.at[4 * part, 1], rem(col + 1, NCOL)
        )

    def wide_copy(stage, buffer, l, way, to):
        return to_col(buffer[l].at[0], buffer[l].at[1 + way], xy_recv.at[stage, l], to[way])

    def half_copy(stage, buffer, l, half, to):
        return to_col(buffer[l].at[0, half], buffer[l].at[1, half], xy_recv.at[stage, l], to[half])

    def shifted(stage, buffer, l):
        part = buffer[l].at[pl.ds(0, 2)] if stage % 2 == 0 else buffer[l].at[0]
        total(part, xy_send, xy_recv.at[stage, l]).wait_recv()

    for l in range(LAYERS):
        if l == 0:
            for part in range(2):
                first_copy(part).start()
        else:
            b_copy(l).start()
        a_copy(l).start()
    for l in range(LAYERS):
        for way in range(2):
            wide_copy(0, y1, l, way, (y_next, y_back)).start()

    def z_copy(way, d, at, slot):
        to = rem(z + (1, NZ - 1)[way], NZ) * 2 + core
        return pltpu.make_async_remote_copy(
            src_ref=g_ref.at[(d, 0) + at], dst_ref=g_ref.at[((d + (NZ - 1, 1)[way]) % NZ, 0) + at],
            send_sem=z_send, recv_sem=z_recv.at[slot],
            device_id=(to, col), device_id_type=MESH,
        )

    def d_copy(d, q, recv):
        return pltpu.make_async_remote_copy(
            src_ref=g_ref.at[d, 0, q], dst_ref=g_ref.at[d, 1, q],
            send_sem=d_send, recv_sem=recv,
            device_id=(z * 2 + 1 - core, col), device_id_type=MESH,
        )

    def send_own(q, half=None):
        at = (q,) if half is None else (q, half)
        for way in range(2):
            z_copy(way, 0, at, q // 4 * 14 + q % 4).start()
        if half != 0:
            d_copy(0, q, own_recv.at[q // 4]).start()

    def own_beside(group):
        total(g_ref.at[0, 0, pl.ds(0, 4)], d_send, own_recv.at[group]).wait_recv()

    def place(way, slot):
        group, i = slot // 14, slot % 14
        hop = i // 4 + 1
        q = group * 4 + (i % 4 if i < 12 else 2 * (i - 12) + way)
        return (NZ - hop, hop)[way], q

    def ring(slot):
        i = slot % 14
        total(g_ref.at[0, 0, pl.ds(0, 2)], z_send, z_recv.at[slot]).wait_recv()
        for way in range(2):
            d, q = place(way, slot)
            if i < 8:
                z_copy(way, d, (q,), slot + 4).start()
            elif i < 12 and i % 2 == way:
                z_copy(way, d, (q,), slot - i + 12 + (i - 8) // 2).start()
        for way in range(2):
            d, q = place(way, slot)
            d_copy(d, q, d_recv.at[slot]).start()

    def beside(slot):
        total(g_ref.at[0, 0, pl.ds(0, 2)], d_send, d_recv.at[slot]).wait_recv()

    def biggest(group):
        rows = []
        for half in range(2):
            for l in range(LAYERS):
                block = g_ref[0, 0, group * 4 + l, half]
                rows.append(jnp.max(jnp.abs(block.astype(jnp.float32)), axis=0, keepdims=True))
        mine_ref[group] = jnp.concatenate(rows, axis=0)

    def mx_copy(group, by):
        return pltpu.make_async_remote_copy(
            src_ref=mine_ref.at[group], dst_ref=mx_ref.at[group, by],
            send_sem=mx_send, recv_sem=mx_recv.at[group],
            device_id=(rem(row + by, 16), col), device_id_type=MESH,
        )

    def settle(group):
        total(mx_ref.at[group, pl.ds(1, 15)], mx_send, mx_recv.at[group]).wait_recv()
        top = mine_ref[group]
        for rb in range(1, 16):
            top = jnp.maximum(top, mx_ref[group, rb])
        top = jnp.broadcast_to(jnp.max(top, axis=1, keepdims=True), top.shape)
        pk_ref[group] = top
        rk_ref[group] = 1.0 / ((top + EPS) * 0.0625)

    even = rem(z, 2) == 0

    def unit(group, t, l):
        p = rem(z // 2 + (0, -1, 1, 2)[t] * (1 - 2 * rem(z, 2)) + 4, 4)
        q = group * 4 + l
        start = pl.multiple_of(p * quad, HDIM)
        for half in range(2):
            scale = rk_ref[group, half * 4 + l:half * 4 + l + 1, :]
            for d in ((0, 1), (-1, -2), (2, 3), (-3, 4))[t]:
                for other in range(2):
                    block = g_ref[d % NZ, other, q, half]
                    if d % 4:
                        block = jnp.where(even, block, g_ref[-d % NZ, other, q, half])
                    at = start + rem(z + d + NZ, 2) * (2 * depth) + (core + other - 2 * core * other) * depth
                    c_ref[q, half, pl.ds(pl.multiple_of(at, 16), depth), :] = (
                        (block.astype(jnp.float32) * 0.0625) * scale
                    ).astype(jnp.bfloat16)
        if group == 1 and t == 3 and l >= 2:
            return
        both = jnp.concatenate(
            [c_ref[q, 0, pl.ds(start, quad), :], c_ref[q, 1, pl.ds(start, quad), :]], axis=1
        )
        acc_ref[q] += jnp.dot(
            probe_ref[:, pl.ds(start, quad)], both, preferred_element_type=jnp.float32
        )

    def took(kind, l):
        (a_copy, b_copy)[kind](l).wait_recv()
        send_own(2 * (1 - kind) + l // 2, l % 2)

    for part in range(2):
        first_copy(part).wait_recv()
        for way in range(2):
            z_copy(way, 0, (0, 0, first_rows(part)), 0).start()
    took(1, 1)
    took(0, 0)
    took(1, 2)
    took(1, 3)
    took(0, 1)
    ring(0)
    took(0, 2)
    beside(0)
    ring(1)
    took(0, 3)
    biggest(0)

    for i in range(2, 15):
        if i == 3:
            for by in range(1, 16):
                mx_copy(0, by).start()
        sends = []
        l = i - 4
        if 0 <= l < 4:
            shifted(0, y1, l)
            y2[l][0, 0] = choose(y1_s, [y1[l][k, 0] for k in range(3)])
            y2[l][0, 1] = choose(y1_e, [y1[l][k, 1] for k in range(3)])
            sends += [half_copy(1, y2, l, half, (y_next, y_back)) for half in range(2)]
        l = i - 7
        if 0 <= l < 4:
            shifted(1, y2, l)
            x1[l][0, 0] = choose(y2_s, [y2[l][k, 0] for k in range(2)])
            x1[l][0, 1] = choose(y2_e, [y2[l][k, 1] for k in range(2)])
            sends += [wide_copy(2, x1, l, way, (x_next, x_back)) for way in range(2)]
        l = i - 9
        if 0 <= l < 4:
            shifted(2, x1, l)
            x2[l][0, 0] = choose(x1_s, [x1[l][k, 0] for k in range(3)])
            x2[l][0, 1] = choose(x1_e, [x1[l][k, 1] for k in range(3)])
            sends += [half_copy(3, x2, l, half, (x_next, x_back)) for half in range(2)]
        l = i - 11
        own = None
        if 0 <= l < 4:
            shifted(3, x2, l)
            g_ref[0, 0, 4 + l, 0] = choose(x2_s, [x2[l][k, 0] for k in range(2)])
            g_ref[0, 0, 4 + l, 1] = choose(x2_e, [x2[l][k, 1] for k in range(2)])
            own = 4 + l
        beside(i - 1)
        for copy in sends:
            copy.start()
        if own is not None:
            send_own(own)
        ring(i)

    p_copy().wait()
    last_ref[...] = probe_ref[:, pl.ds(pl.multiple_of(rem(z // 2 + 2, 4) * quad, HDIM), quad)]
    biggest(1)
    settle(0)
    own_beside(0)

    for by in range(1, 16):
        mx_copy(1, by).start()

    def units(group, t, first, last):
        for l in range(first, last):
            unit(group, t, l)

    work = {15: (0, 0, 0, 4), 16: (0, 1, 0, 4), 17: (0, 2, 0, 4), 18: (0, 3, 0, 4)}
    work.update({21: (1, 0, 0, 4), 22: (1, 1, 0, 4), 24: (1, 2, 0, 2), 26: (1, 2, 2, 4)})
    work.update({27: (1, 3, 0, 2), 28: (1, 3, 2, 4)})
    for slot in range(15, 29):
        beside(slot - 1)
        if slot < 28:
            ring(slot)
        if slot == 21:
            settle(1)
            own_beside(1)
        if slot in work:
            units(*work[slot])

    total(g_ref.at[pl.ds(0, 7), 0], z_send, z_recv.at[0]).wait_send()
    total(g_ref.at[pl.ds(0, 8), 0], d_send, z_recv.at[0]).wait_send()
    total(g_ref.at[pl.ds(0, 7), 0, pl.ds(0, 4)], xy_send, z_recv.at[0]).wait_send()
    total(mx_ref.at[pl.ds(0, 2), pl.ds(1, 15)], mx_send, mx_recv.at[0]).wait_send()


def piece(l, c):
    if c < 2:
        return 2 * (1 - c) + l // 2, l % 2
    return 4 + l, c - 2


def output_kernel(
    src_ref, tgt_ref, c_ref, acc_ref, pk_ref, last_ref,
    codes_hbm, peaks_ref, checked_hbm,
    chk_ref, sem, chk_sem,
):
    col = lax.axis_index("col")
    z = lax.axis_index("row") // 2
    quad = c_ref.shape[2] // 4
    classes = recv_classes(src_ref, tgt_ref, col)
    slots = []
    for c in range(4):
        at = jnp.int32(0)
        for j in range(1, PER):
            at = jnp.where(classes[j] == c, j, at)
        slots.append(at)

    def lanes(c):
        return pl.ds(pl.multiple_of(slots[c] * HDIM, HDIM), HDIM)

    copies = []
    for l in range(LAYERS):
        for c in range(4):
            copy = pltpu.make_async_copy(
                c_ref.at[piece(l, c)], codes_hbm.at[l, :, lanes(c)], sem.at[l, c]
            )
            copy.start()
            copies.append(copy)
    start = pl.multiple_of(rem(z // 2 + 2, 4) * quad, HDIM)

    def put(l, c, block):
        q, half = piece(l, c)
        scale = pk_ref[q // 4, half * 4 + q % 4:half * 4 + q % 4 + 1, :]
        chk_ref[l, c] = (block * scale).astype(jnp.bfloat16)
        copy = pltpu.make_async_copy(
            chk_ref.at[l, c], checked_hbm.at[l, :, lanes(c)], chk_sem.at[l, c]
        )
        copy.start()
        copies.append(copy)

    for l in range(LAYERS):
        for c in range(2):
            q, half = piece(l, c)
            put(l, c, acc_ref[q, :, half * HDIM:(half + 1) * HDIM])
    for l in range(LAYERS):
        last = acc_ref[4 + l]
        if l >= 2:
            both = jnp.concatenate(
                [c_ref[4 + l, 0, pl.ds(start, quad), :], c_ref[4 + l, 1, pl.ds(start, quad), :]], axis=1
            )
            last = last + jnp.dot(last_ref[...], both, preferred_element_type=jnp.float32)
        for c in range(2, 4):
            put(l, c, last[:, (c - 2) * HDIM:(c - 1) * HDIM])
    lane = lax.broadcasted_iota(jnp.int32, (LAYERS, HDIM), 1)
    out = jnp.zeros((LAYERS, HDIM), jnp.float32)
    for c in range(4):
        rows = []
        for l in range(LAYERS):
            q, half = piece(l, c)
            rows.append(pk_ref[q // 4, half * 4 + q % 4:half * 4 + q % 4 + 1, :])
        out = jnp.where(lane == slots[c], jnp.concatenate(rows, axis=0), out)
    peaks_ref[...] = out[:, :PER]
    for copy in copies:
        copy.wait()


def per_device(train_weight, src_map, tgt_map, probe):
    layers, depth, width = train_weight.shape
    tokens, model = probe.shape
    bf16, f32 = jnp.bfloat16, jnp.float32
    smem = pl.BlockSpec(memory_space=pltpu.SMEM)
    vmem = pl.BlockSpec(memory_space=pltpu.VMEM)
    hbm = pl.BlockSpec(memory_space=pl.ANY)
    three = pltpu.VMEM((3, 2, depth, HDIM), bf16)
    two = pltpu.VMEM((2, 2, depth, HDIM), bf16)
    dma = pltpu.SemaphoreType.DMA
    c, acc, pk, held = pl.pallas_call(
        gather_kernel,
        name="gather_codes",
        out_shape=(
            pltpu.VMEM((8, 2, model, HDIM), bf16),
            pltpu.VMEM((8, tokens, 2 * HDIM), f32),
            pltpu.VMEM((2, 8, HDIM), f32),
            pltpu.VMEM((tokens, model // 4), bf16),
        ),
        in_specs=[smem, smem, hbm, hbm],
        out_specs=(vmem, vmem, vmem, vmem),
        scratch_shapes=[
            pltpu.VMEM((NZ, 2, 8, 2, depth, HDIM), bf16),
            pltpu.VMEM((tokens, model), bf16),
            pltpu.VMEM((layers, depth, width), bf16),
            pltpu.VMEM((layers, 2, depth, HDIM), bf16),
            pltpu.VMEM((2, 16, 8, HDIM), f32),
            pltpu.VMEM((2, 8, HDIM), f32),
            pltpu.VMEM((2, 8, HDIM), f32),
        ]
        + [three] * 4 + [two] * 4 + [three] * 4 + [two] * 4
        + [
            dma((4,)), dma, dma((5, 2)), dma((4, 4)), dma((28,)), dma((2,)), dma((28,)), dma((2,)),
            dma, dma, dma, dma,
        ],
        compiler_params=pltpu.CompilerParams(
            collective_id=0, has_side_effects=True, vmem_limit_bytes=34 * 1024 * 1024
        ),
    )(src_map, tgt_map, train_weight, probe)
    return pl.pallas_call(
        output_kernel,
        name="write_outputs",
        out_shape=(
            jax.ShapeDtypeStruct((layers, model, width), bf16),
            jax.ShapeDtypeStruct((layers, PER), f32),
            jax.ShapeDtypeStruct((layers, tokens, width), bf16),
        ),
        in_specs=[smem, smem, vmem, vmem, vmem, vmem],
        out_specs=(hbm, vmem, hbm),
        scratch_shapes=[
            pltpu.VMEM((layers, 4, tokens, HDIM), bf16),
            dma((4, 4)),
            dma((4, 4)),
        ],
        compiler_params=pltpu.CompilerParams(vmem_limit_bytes=4 * 1024 * 1024),
    )(src_map, tgt_map, c, acc, pk, held)


def solution(mesh):
    in_specs = (P(None, "row", "col"), P(), P(), P("row", None))
    out_specs = (P(None, None, "col"), P(None, "col"), P(None, "row", "col"))
    return jax.shard_map(
        per_device, mesh=mesh, in_specs=in_specs, out_specs=out_specs, check_vma=False
    )
```
